32 devices in a mesh: section: 8 (over y, x, core), tensor: 4 (over z).
Axes of the slice: x: 2, y: 2, z: 4, core: 2. Of those that a mesh axis runs over, the one named last changes fastest.
Arguments:
- section_inputs: bfloat16 [8, 512, 1024], P('section', 'tensor'), may hold values from -6 to 6
- w_in: bfloat16 [8, 2304, 1024], P('section', 'tensor'), may hold values from -0.1875 to 0.1875
- in_bias: bfloat16 [8, 2304], P('section', 'tensor'), may hold values from -3 to 3
- w_out: bfloat16 [8, 2304, 1024], P('section', 'tensor'), may hold values from -0.125 to 0.125
- out_bias: float32 [8, 1024], P('section'), may hold values from -2 to 2
- norm_gain: float32 [8, 1024], P('section'), may hold values from 0.1 to 1.9
- norm_bias: float32 [8, 1024], P('section'), may hold values from -2 to 2
- patches: bfloat16 [8, 512, 1024], P(None, 'tensor'), may hold values from -6 to 6
- plan: int32 [3], replicated, may hold values from 0 to 7, as said below
Outputs:
- received: bfloat16 [8, 4, 512, 1024], P('section', None, 'tensor')
The draws below stay inside these ranges and needn't reach their ends.
Inputs may be any that keep to these rules, and one draw needn't show every extreme that they name: `plan`: the first min(8, 3) entries are all different.
All inputs are finite; a program needn't handle non-finite values.
Results may differ from the reference program's by a relative error of at most 0.0065.
Values may be sent and summed in bfloat16 or wider, within the bound.
No kernel may reach another device: no remote copies, remote signals or barrier semaphores. Data moves between devices by JAX's collectives and lax.ppermute only.
A program may use at most 64 MiB of HBM per device.

```python
import jax
import jax.numpy as jnp
from jax import lax

D = 1024
FF = 2304
TICKS = 4
MICRO = 8
TOKG = 512
N_SECTION = 8


def draw_plan(key, part):
    order = jax.random.permutation(key, MICRO).astype(jnp.int32)
    places = jnp.arange(TICKS - 1, dtype=jnp.int32) % MICRO
    return order[places].astype(jnp.int32)


def block_scale(key, shape, shards, least, largest):
    def one(position, parts):
        heights = jax.random.uniform(jax.random.fold_in(jax.random.fold_in(key, 6), position), (parts,), jnp.float32, least / len(shards), largest / len(shards))
        return jnp.repeat(jnp.exp(heights), shape[position] // parts).reshape((-1,) + (1,) * (len(shape) - position - 1))

    level = one(*shards[0])
    for cut in shards[1:]:
        level = level * one(*cut)
    return level


def noise(own_key, shape, scale, reach, shards=(), held_as=jnp.bfloat16):
    factor_of = block_scale(own_key, shape, shards, -0.22, 0.18) if shards else 1.0
    array = jax.random.normal(own_key, shape, jnp.float32) * scale * factor_of
    return jnp.minimum(jnp.maximum(array, -reach), reach).astype(held_as)


def setup_inputs(seed: int = 0) -> dict:
    key_of = jax.random.split(jax.random.key(seed), 10)
    section_inputs = noise(key_of[0], (N_SECTION, TOKG, D), 1.0, 6.0, ((0, 8), (1, 4)))
    w_in = noise(key_of[1], (N_SECTION, FF, D), D ** -0.5, 0.1875, ((0, 8), (1, 4)))
    in_bias = noise(key_of[2], (N_SECTION, FF), 0.5, 3.0, ((0, 8), (1, 4)))
    w_out = noise(key_of[3], (N_SECTION, FF, D), FF ** -0.5, 0.125, ((0, 8), (1, 4)))
    out_bias = noise(key_of[4], (N_SECTION, D), 0.3, 2.0, ((0, 8),), jnp.float32)
    norm_gain = jnp.clip(1.0 + 0.18 * jax.random.normal(key_of[5], (N_SECTION, D), jnp.float32), 0.1, 1.9)
    norm_bias = noise(key_of[6], (N_SECTION, D), 0.3, 2.0, ((0, 8),), jnp.float32)
    patches = noise(key_of[7], (MICRO, TOKG, D), 1.0, 6.0, ((1, 4),))
    plan = draw_plan(jax.random.fold_in(key_of[9], 71), 0)
    return {"section_inputs": section_inputs, "w_in": w_in, "in_bias": in_bias, "w_out": w_out, "out_bias": out_bias, "norm_gain": norm_gain, "norm_bias": norm_bias, "patches": patches, "plan": plan}


norm_floor = 0.1
gelu_slope = 1.702

def normalize(current, gain_row, shift_row):
    widened = current.astype(jnp.float32)
    average = lax.optimization_barrier(jnp.mean(widened, axis=-1, keepdims=True))
    centered = widened - average
    variance = lax.optimization_barrier(jnp.mean(centered * centered, axis=-1, keepdims=True))
    normed = (centered * lax.rsqrt(variance + norm_floor) * gain_row + shift_row).astype(jnp.bfloat16)
    return (normed, widened)

def activate(preact):
    return preact * jax.nn.sigmoid(gelu_slope * preact)

def apply_block(current, gain_row, shift_row, full_in, full_bias, full_out, bias_row):
    normed, widened = normalize(current, gain_row, shift_row)
    preact = lax.dot_general(normed, full_in, (((1,), (1,)), ((), ())), preferred_element_type=jnp.float32)
    preact = preact + full_bias.astype(jnp.float32)
    hidden = activate(preact).astype(jnp.bfloat16)
    return (widened + jnp.dot(hidden, full_out, preferred_element_type=jnp.float32) + bias_row).astype(jnp.bfloat16)

def reference(section_inputs, w_in, in_bias, w_out, out_bias, norm_gain, norm_bias, patches, plan):
    current = section_inputs
    records = []
    for tick_index in range(TICKS):
        produced = lax.map(lambda operands: apply_block(*operands), (current, norm_gain, norm_bias, w_in, in_bias, w_out, out_bias))
        arrived = jnp.roll(produced, 1, axis=0)
        records.append(arrived)
        if tick_index + 1 < TICKS:
            selected = lax.dynamic_index_in_dim(patches, plan[tick_index], 0, keepdims=False)
            current = arrived.at[0].set(selected)
    return jnp.stack(records, axis=1)
```

```python
import jax
import jax.numpy as jnp
from jax import lax
from jax.sharding import PartitionSpec as P

TICKS = 4


norm_floor = 0.1
gelu_slope = 1.702


class Plan:
    def __init__(self, sections, tensors):
        self.sections = sections
        self.tensors = tensors
        self.half = tensors // 2

    def side(self, section):
        return (section // 2 + section) % 2

    def stage(self, section):
        return self.half - 1 + self.side(section)

    def device(self, section, tensor):
        return section * self.tensors + tensor

    def worker(self, section, core):
        return self.device(section // 2 * 2 + core, self.stage(section))

    def weight_pairs(self, slot):
        pairs = []
        for section in range(self.sections):
            for step in (2 * slot, 2 * slot + 1):
                shard = (self.stage(section) + step) % self.tensors
                pairs.append(
                    (self.device(section, shard), self.worker(section, (section + step) % 2))
                )
        return pairs

    def token_pairs(self, slot, sections):
        return [
            (self.device(section, core * self.half + slot), self.worker(section, core))
            for section in sections
            for core in range(2)
        ]

    def partner_pairs(self):
        return [
            (self.worker(section, core), self.worker(section, 1 - core))
            for section in range(self.sections)
            for core in range(2)
        ]

    def hop_pairs(self):
        return [
            (self.worker(section, core), self.worker((section + 1) % self.sections, core))
            for section in range(self.sections)
            for core in range(2)
        ]

    def home_pairs(self, slot, shift):
        return [
            (
                self.worker((section - shift) % self.sections, core),
                self.device(section, core * self.half + slot),
            )
            for section in range(self.sections)
            for core in range(2)
        ]


def send(value, pairs):
    return lax.ppermute(value, ("section", "tensor"), pairs)


def normalize(current, gain_row, shift_row):
    widened = current.astype(jnp.float32)
    average = jnp.mean(widened, axis=-1, keepdims=True)
    centered = widened - average
    variance = jnp.mean(centered * centered, axis=-1, keepdims=True)
    normed = (centered * lax.rsqrt(variance + norm_floor) * gain_row + shift_row).astype(
        jnp.bfloat16
    )
    return (normed, widened)


def activate(preact):
    return preact * jax.nn.sigmoid(gelu_slope * preact)


def apply_block(current, weights, gain_row, shift_row, bias_row):
    normed, widened = normalize(current, gain_row, shift_row)
    total = None
    for rows_in, rows_bias, rows_out in weights:
        preact = lax.dot_general(
            normed, rows_in, (((1,), (1,)), ((), ())), preferred_element_type=jnp.float32
        )
        hidden = activate(preact + rows_bias).astype(jnp.bfloat16)
        part = jnp.dot(hidden, rows_out, preferred_element_type=jnp.float32)
        total = part if total is None else total + part
    return (widened + total + bias_row).astype(jnp.bfloat16)


def collapsed(section_inputs, w_in, in_bias, w_out, out_bias, norm_gain, norm_bias, patches, plan):
    places = Plan(lax.axis_size("section"), lax.axis_size("tensor"))
    tensors, half = places.tensors, places.half
    section_index = lax.axis_index("section")
    tensor_index = lax.axis_index("tensor")
    core = section_index % 2
    line = section_index // 2
    side = (tensor_index >= half).astype(jnp.int32)
    own_core = (line + side) % 2
    is_own = core == own_core
    is_first = (line == 0) & (own_core == 0)

    everyone = range(places.sections)
    slots = range(half)
    currents = [send(section_inputs[0], places.token_pairs(slot, everyone)) for slot in slots]

    weights_in = [send(w_in[0], places.weight_pairs(slot)) for slot in slots]
    weights_out = [send(w_out[0], places.weight_pairs(slot)) for slot in slots]

    biases = [in_bias] + [
        lax.ppermute(
            in_bias, "tensor", [((place + step) % tensors, place) for place in range(tensors)]
        )
        for step in range(1, tensors)
    ]
    bias_table = jnp.concatenate(biases, axis=0).astype(jnp.float32)
    rows = jnp.concatenate([norm_gain, norm_bias, out_bias], axis=0)
    partner = places.partner_pairs()
    bias_table = jnp.where(is_own, bias_table, send(bias_table, partner))
    rows = jnp.where(is_own, rows, send(rows, partner))
    gain_row, shift_row, bias_row = rows[0:1], rows[1:2], rows[2:3]

    weights = []
    for slot in slots:
        even, odd = bias_table[2 * slot][None], bias_table[2 * slot + 1][None]
        weights.append(
            (weights_in[slot], jnp.where(is_own, even, odd), weights_out[slot])
        )
        weights.append(
            (
                send(weights_in[slot], partner),
                jnp.where(is_own, odd, even),
                send(weights_out[slot], partner),
            )
        )

    records = []
    for tick_index in range(TICKS):
        last = tick_index + 1 == TICKS
        produced = [
            apply_block(current, weights, gain_row, shift_row, bias_row) for current in currents
        ]
        if last:
            pieces = [send(produced[slot], places.home_pairs(slot, 1)) for slot in slots]
        else:
            selected = lax.dynamic_index_in_dim(patches, plan[tick_index], 0, keepdims=False)
            selected, _ = lax.optimization_barrier((selected, produced[0]))
            fresh = [send(selected, places.token_pairs(slot, [0])) for slot in slots]
            arrived = [send(produced[slot], places.hop_pairs()) for slot in slots]
            pieces = [send(arrived[slot], places.home_pairs(slot, 0)) for slot in slots]
            currents = [jnp.where(is_first, fresh[slot], arrived[slot]) for slot in slots]
        mine = pieces[0]
        for slot in range(1, half):
            mine = jnp.where(tensor_index % half == slot, pieces[slot], mine)
        records.append(mine)
    return jnp.stack(records, axis=0)[None]


def gathered(section_inputs, w_in, in_bias, w_out, out_bias, norm_gain, norm_bias, patches, plan):
    sections = lax.axis_size("section")
    section_index = lax.axis_index("section")
    gather = lambda value: lax.all_gather(value, "tensor", axis=0, tiled=True)
    full_in, full_bias, full_out = gather(w_in[0]), gather(in_bias[0]), gather(w_out[0])
    weights = [(full_in, full_bias.astype(jnp.float32), full_out)]
    current = section_inputs[0]
    records = []
    for tick_index in range(TICKS):
        produced = apply_block(current, weights, norm_gain[0], norm_bias[0], out_bias[0])
        pairs = [(source, (source + 1) % sections) for source in range(sections)]
        arrived = lax.ppermute(produced, "section", pairs)
        records.append(arrived)
        if tick_index + 1 < TICKS:
            selected = lax.dynamic_index_in_dim(patches, plan[tick_index], 0, keepdims=False)
            current = jnp.where(section_index == 0, selected, arrived)
    return jnp.stack(records, axis=0)[None]


def solution(mesh):
    sections, tensors = mesh.shape["section"], mesh.shape["tensor"]
    fits = sections % 2 == 0 and tensors % 2 == 0 and tensors <= sections // 2
    placed = (
        P("section", "tensor", None),
        P("section", "tensor", None),
        P("section", "tensor"),
        P("section", "tensor", None),
        P("section", None),
        P("section", None),
        P("section", None),
        P(None, "tensor", None),
        P(),
    )
    return jax.shard_map(
        collapsed if fits else gathered,
        mesh=mesh,
        in_specs=placed,
        out_specs=P("section", None, "tensor", None),
        check_vma=False,
    )
```

```python
import functools

import jax
import jax.numpy as jnp
from jax import lax
from jax.experimental import pallas as pl
from jax.experimental.pallas import tpu as pltpu
from jax.sharding import PartitionSpec as P

TICKS = 4


norm_floor = 0.1
gelu_slope = 1.702


class Plan:
    def __init__(self, sections, tensors):
        self.sections = sections
        self.tensors = tensors
        self.half = tensors // 2

    def side(self, section):
        return (section // 2 + section) % 2

    def stage(self, section):
        return self.half - 1 + self.side(section)

    def device(self, section, tensor):
        return section * self.tensors + tensor

    def worker(self, section, core):
        return self.device(section // 2 * 2 + core, self.stage(section))

    def weight_pairs(self, slot):
        pairs = []
        for section in range(self.sections):
            for step in (2 * slot, 2 * slot + 1):
                shard = (self.stage(section) + step) % self.tensors
                pairs.append(
                    (self.device(section, shard), self.worker(section, (section + step) % 2))
                )
        return pairs

    def token_pairs(self, slot, sections):
        return [
            (self.device(section, core * self.half + slot), self.worker(section, core))
            for section in sections
            for core in range(2)
        ]

    def partner_pairs(self):
        return [
            (self.worker(section, core), self.worker(section, 1 - core))
            for section in range(self.sections)
            for core in range(2)
        ]

    def hop_pairs(self):
        return [
            (self.worker(section, core), self.worker((section + 1) % self.sections, core))
            for section in range(self.sections)
            for core in range(2)
        ]

    def home_pairs(self, slot, shift):
        return [
            (
                self.worker((section - shift) % self.sections, core),
                self.device(section, core * self.half + slot),
            )
            for section in range(self.sections)
            for core in range(2)
        ]


def send(value, pairs):
    return lax.ppermute(value, ("section", "tensor"), pairs)


def normalize(current, gain_row, shift_row):
    widened = current.astype(jnp.float32)
    average = jnp.mean(widened, axis=-1, keepdims=True)
    centered = widened - average
    variance = jnp.mean(centered * centered, axis=-1, keepdims=True)
    normed = (centered * lax.rsqrt(variance + norm_floor) * gain_row + shift_row).astype(
        jnp.bfloat16
    )
    return (normed, widened)


def activate(preact):
    return preact * jax.nn.sigmoid(gelu_slope * preact)


def apply_block(current, weights, gain_row, shift_row, bias_row):
    normed, widened = normalize(current, gain_row, shift_row)
    total = None
    for rows_in, rows_bias, rows_out in weights:
        preact = lax.dot_general(
            normed, rows_in, (((1,), (1,)), ((), ())), preferred_element_type=jnp.float32
        )
        hidden = activate(preact + rows_bias).astype(jnp.bfloat16)
        part = jnp.dot(hidden, rows_out, preferred_element_type=jnp.float32)
        total = part if total is None else total + part
    return (widened + total + bias_row).astype(jnp.bfloat16)


def block_kernel(first_row, flag, arrived, fresh, rows, bias, rows_in, rows_out, produced):
    new = fresh[first_row : first_row + arrived.shape[0], :]
    current = jnp.where(flag[0] == 1, new, arrived[...])
    normed, widened = normalize(current, rows[0:1, :], rows[1:2, :])
    preact = lax.dot_general(
        normed, rows_in[...], (((1,), (1,)), ((), ())), preferred_element_type=jnp.float32
    )
    hidden = activate(preact + bias[...]).astype(jnp.bfloat16)
    total = jnp.dot(hidden, rows_out[...], preferred_element_type=jnp.float32)
    produced[...] = (widened + total + rows[2:3, :]).astype(jnp.bfloat16)


def run_block(first_row, flag, arrived, fresh, rows, bias, full_in, full_out):
    vector = pl.BlockSpec(memory_space=pltpu.VMEM)
    return pl.pallas_call(
        functools.partial(block_kernel, first_row),
        out_shape=jax.ShapeDtypeStruct(arrived.shape, arrived.dtype),
        in_specs=[pl.BlockSpec(memory_space=pltpu.SMEM)] + [vector] * 6,
        out_specs=vector,
        compiler_params=pltpu.CompilerParams(vmem_limit_bytes=8 * 2**20),
        name="section_block",
    )(flag, arrived, fresh, rows, bias, full_in, full_out)


def collect_kernel(ticks, slots, choice, *refs):
    pieces, records, done = refs[:-2], refs[-2], refs[-1]
    for slot in range(slots):

        @pl.when(choice[0] == slot)
        def _():
            copies = [
                pltpu.make_async_copy(pieces[tick * slots + slot], records.at[tick], done.at[tick])
                for tick in range(ticks)
            ]
            for copy in copies:
                copy.start()
            for copy in copies:
                copy.wait()


def collect(choice, pieces, slots):
    anywhere = pl.BlockSpec(memory_space=pl.ANY)
    ticks = len(pieces) // slots
    return pl.pallas_call(
        functools.partial(collect_kernel, ticks, slots),
        out_shape=jax.ShapeDtypeStruct((ticks,) + pieces[0].shape, pieces[0].dtype),
        in_specs=[pl.BlockSpec(memory_space=pltpu.SMEM)] + [anywhere] * len(pieces),
        out_specs=anywhere,
        scratch_shapes=[pltpu.SemaphoreType.DMA((ticks,))],
        name="collect_quarters",
    )(choice, *pieces)


def after(value, *others):
    return lax.optimization_barrier((value,) + others)[0]


def collapsed(section_inputs, w_in, in_bias, w_out, out_bias, norm_gain, norm_bias, patches, plan):
    places = Plan(lax.axis_size("section"), lax.axis_size("tensor"))
    tensors, half = places.tensors, places.half
    section_index = lax.axis_index("section")
    tensor_index = lax.axis_index("tensor")
    core = section_index % 2
    line = section_index // 2
    side = (tensor_index >= half).astype(jnp.int32)
    own_core = (line + side) % 2
    is_own = core == own_core
    is_first = ((line == 0) & (own_core == 0)).astype(jnp.int32)[None]

    slots = range(half)
    weights_in = [send(w_in[0], places.weight_pairs(slot)) for slot in slots]
    weights_out = [send(w_out[0], places.weight_pairs(slot)) for slot in slots]
    everyone = range(places.sections)
    currents = [send(section_inputs[0], places.token_pairs(slot, everyone)) for slot in slots]

    small = after(in_bias, *weights_in)
    biases = [small] + [
        lax.ppermute(
            small, "tensor", [((place + step) % tensors, place) for place in range(tensors)]
        )
        for step in range(1, tensors)
    ]
    bias_table = jnp.concatenate(biases, axis=0).astype(jnp.float32)
    rows = after(jnp.concatenate([norm_gain, norm_bias, out_bias], axis=0), *weights_in)
    partner = places.partner_pairs()
    bias_table = jnp.where(is_own, bias_table, send(bias_table, partner))
    rows = jnp.where(is_own, rows, send(rows, partner))

    pieces_in, pieces_bias, pieces_out = [], [], []
    for slot in slots:
        even, odd = bias_table[2 * slot], bias_table[2 * slot + 1]
        pieces_in += [weights_in[slot], send(weights_in[slot], partner)]
        pieces_bias += [jnp.where(is_own, even, odd), jnp.where(is_own, odd, even)]
        pieces_out += [weights_out[slot], send(weights_out[slot], partner)]
    full_in = jnp.concatenate(pieces_in, axis=0)
    full_out = jnp.concatenate(pieces_out, axis=0)
    bias = jnp.concatenate(pieces_bias, axis=0)[None]

    selected = jnp.concatenate(
        [
            lax.dynamic_index_in_dim(patches, plan[tick_index], 0, keepdims=False)
            for tick_index in range(TICKS - 1)
        ],
        axis=0,
    )
    selected = after(selected, *weights_out)
    waiting = [send(selected, places.token_pairs(slot, [0])) for slot in slots]
    chunk = section_inputs.shape[1]

    pieces = []
    flag, fresh, first_row = jnp.zeros_like(is_first), currents, 0
    for tick_index in range(TICKS):
        produced = [
            run_block(first_row, flag, currents[slot], fresh[slot], rows, bias, full_in, full_out)
            for slot in slots
        ]
        if tick_index + 1 == TICKS:
            pieces += [send(produced[slot], places.home_pairs(slot, 1)) for slot in slots]
        else:
            currents = [send(produced[slot], places.hop_pairs()) for slot in slots]
            pieces += [send(currents[slot], places.home_pairs(slot, 0)) for slot in slots]
            flag, fresh, first_row = is_first, waiting, tick_index * chunk
    return collect((tensor_index % half)[None], pieces, half)[None]


def gathered(section_inputs, w_in, in_bias, w_out, out_bias, norm_gain, norm_bias, patches, plan):
    sections = lax.axis_size("section")
    section_index = lax.axis_index("section")
    gather = lambda value: lax.all_gather(value, "tensor", axis=0, tiled=True)
    full_in, full_bias, full_out = gather(w_in[0]), gather(in_bias[0]), gather(w_out[0])
    weights = [(full_in, full_bias.astype(jnp.float32), full_out)]
    current = section_inputs[0]
    records = []
    for tick_index in range(TICKS):
        produced = apply_block(current, weights, norm_gain[0], norm_bias[0], out_bias[0])
        pairs = [(source, (source + 1) % sections) for source in range(sections)]
        arrived = lax.ppermute(produced, "section", pairs)
        records.append(arrived)
        if tick_index + 1 < TICKS:
            selected = lax.dynamic_index_in_dim(patches, plan[tick_index], 0, keepdims=False)
            current = jnp.where(section_index == 0, selected, arrived)
    return jnp.stack(records, axis=0)[None]


def solution(mesh):
    sections, tensors = mesh.shape["section"], mesh.shape["tensor"]
    fits = sections % 2 == 0 and tensors % 2 == 0 and tensors <= sections // 2
    placed = (
        P("section", "tensor", None),
        P("section", "tensor", None),
        P("section", "tensor"),
        P("section", "tensor", None),
        P("section", None),
        P("section", None),
        P("section", None),
        P(None, "tensor", None),
        P(),
    )
    return jax.shard_map(
        collapsed if fits else gathered,
        mesh=mesh,
        in_specs=placed,
        out_specs=P("section", None, "tensor", None),
        check_vma=False,
    )
```

```python
import functools

import jax
import jax.numpy as jnp
from jax import lax
from jax.experimental import pallas as pl
from jax.experimental.pallas import tpu as pltpu
from jax.sharding import PartitionSpec as P

TICKS = 4


norm_floor = 0.1
gelu_slope = 1.702


class Plan:
    def __init__(self, sections, tensors):
        self.sections = sections
        self.tensors = tensors
        self.half = tensors // 2

    def side(self, section):
        return (section // 2 + section) % 2

    def stage(self, section):
        return self.half - 1 + self.side(section)

    def device(self, section, tensor):
        return section * self.tensors + tensor

    def worker(self, section, core):
        return self.device(section // 2 * 2 + core, self.stage(section))

    def weight_pairs(self, slot):
        return [
            (
                self.device(section, (self.stage(section) + step) % self.tensors),
                self.worker(section, (section + step) % 2),
            )
            for section in range(self.sections)
            for step in (2 * slot, 2 * slot + 1)
            if step > 0
        ]

    def own_pairs(self, back):
        pairs = [
            (self.worker(section, section % 2), self.worker(section, 1 - section % 2))
            for section in range(self.sections)
        ]
        return [(target, source) for source, target in pairs] if back else pairs

    def token_pairs(self, slot, sections):
        return [
            (self.device(section, core * self.half + slot), self.worker(section, core))
            for section in sections
            for core in range(2)
        ]

    def partner_pairs(self):
        return [
            (self.worker(section, core), self.worker(section, 1 - core))
            for section in range(self.sections)
            for core in range(2)
        ]

    def hop_pairs(self):
        return [
            (self.worker(section, core), self.worker((section + 1) % self.sections, core))
            for section in range(self.sections)
            for core in range(2)
        ]

    def home_pairs(self, slot, shift):
        return [
            (
                self.worker((section - shift) % self.sections, core),
                self.device(section, core * self.half + slot),
            )
            for section in range(self.sections)
            for core in range(2)
        ]


def send(value, pairs):
    return lax.ppermute(value, ("section", "tensor"), pairs)


def normalize(current, gain_row, shift_row):
    widened = current.astype(jnp.float32)
    average = jnp.mean(widened, axis=-1, keepdims=True)
    centered = widened - average
    variance = jnp.mean(centered * centered, axis=-1, keepdims=True)
    normed = (centered * lax.rsqrt(variance + norm_floor) * gain_row + shift_row).astype(
        jnp.bfloat16
    )
    return (normed, widened)


def activate(preact):
    return preact * jax.nn.sigmoid(gelu_slope * preact)


def apply_block(current, weights, gain_row, shift_row, bias_row):
    normed, widened = normalize(current, gain_row, shift_row)
    total = None
    for rows_in, rows_bias, rows_out in weights:
        preact = lax.dot_general(
            normed, rows_in, (((1,), (1,)), ((), ())), preferred_element_type=jnp.float32
        )
        hidden = activate(preact + rows_bias).astype(jnp.bfloat16)
        part = jnp.dot(hidden, rows_out, preferred_element_type=jnp.float32)
        total = part if total is None else total + part
    return (widened + total + bias_row).astype(jnp.bfloat16)


def block_kernel(first_row, flag, arrived, fresh, rows, bias, rows_in, rows_out, produced):
    new = fresh[first_row : first_row + arrived.shape[0], :]
    current = jnp.where(flag[0] == 1, new, arrived[...])
    normed, widened = normalize(current, rows[0:1, :], rows[1:2, :])
    preact = lax.dot_general(
        normed, rows_in[...], (((1,), (1,)), ((), ())), preferred_element_type=jnp.float32
    )
    hidden = activate(preact + bias[...]).astype(jnp.bfloat16)
    total = jnp.dot(hidden, rows_out[...], preferred_element_type=jnp.float32)
    produced[...] = (widened + total + rows[2:3, :]).astype(jnp.bfloat16)


def run_block(first_row, flag, arrived, fresh, rows, bias, full_in, full_out):
    vector = pl.BlockSpec(memory_space=pltpu.VMEM)
    return pl.pallas_call(
        functools.partial(block_kernel, first_row),
        out_shape=jax.ShapeDtypeStruct(arrived.shape, arrived.dtype),
        in_specs=[pl.BlockSpec(memory_space=pltpu.SMEM)] + [vector] * 6,
        out_specs=vector,
        compiler_params=pltpu.CompilerParams(vmem_limit_bytes=8 * 2**20),
        name="section_block",
    )(flag, arrived, fresh, rows, bias, full_in, full_out)


def collect_kernel(choice, *refs):
    pieces, records = refs[:-1], refs[-1]
    ticks = records.shape[0]
    slots = len(pieces) // ticks
    for tick in range(ticks):
        mine = pieces[tick * slots][...]
        for slot in range(1, slots):
            mine = jnp.where(choice[0] == slot, pieces[tick * slots + slot][...], mine)
        records[tick] = mine


def collect(choice, pieces, slots):
    vector = pl.BlockSpec(memory_space=pltpu.VMEM)
    ticks = len(pieces) // slots
    return pl.pallas_call(
        collect_kernel,
        out_shape=jax.ShapeDtypeStruct((ticks,) + pieces[0].shape, pieces[0].dtype),
        in_specs=[pl.BlockSpec(memory_space=pltpu.SMEM)] + [vector] * len(pieces),
        out_specs=vector,
        compiler_params=pltpu.CompilerParams(vmem_limit_bytes=8 * 2**20),
        name="collect_quarters",
    )(choice, *pieces)


def assemble_kernel(flag, *refs):
    here, there, full, done = refs[: len(refs) // 2 - 1], refs[len(refs) // 2 - 1 : -2], refs[-2], refs[-1]
    size = here[0].shape[0]

    def place(parts):
        copies = [
            pltpu.make_async_copy(part, full.at[pl.ds(step * size, size)], done.at[step])
            for step, part in enumerate(parts)
        ]
        for copy in copies:
            copy.start()
        for copy in copies:
            copy.wait()

    @pl.when(flag[0] == 1)
    def _():
        place(here)

    @pl.when(flag[0] == 0)
    def _():
        place(there)


def assemble(flag, own, partner):
    anywhere = pl.BlockSpec(memory_space=pl.ANY)
    size, width = own[0].shape
    return pl.pallas_call(
        assemble_kernel,
        out_shape=jax.ShapeDtypeStruct((size * len(own), width), own[0].dtype),
        in_specs=[pl.BlockSpec(memory_space=pltpu.SMEM)] + [anywhere] * (2 * len(own)),
        out_specs=pl.BlockSpec(memory_space=pltpu.VMEM),
        scratch_shapes=[pltpu.SemaphoreType.DMA((len(own),))],
        compiler_params=pltpu.CompilerParams(vmem_limit_bytes=8 * 2**20),
        name="assemble_shards",
    )(flag, *own, *partner)


def after(value, *others):
    return lax.optimization_barrier((value,) + others)[0]


def collapsed(section_inputs, w_in, in_bias, w_out, out_bias, norm_gain, norm_bias, patches, plan):
    places = Plan(lax.axis_size("section"), lax.axis_size("tensor"))
    tensors, half = places.tensors, places.half
    section_index = lax.axis_index("section")
    tensor_index = lax.axis_index("tensor")
    core = section_index % 2
    line = section_index // 2
    side = (tensor_index >= half).astype(jnp.int32)
    own_core = (line + side) % 2
    is_own = core == own_core
    is_first = ((line == 0) & (own_core == 0)).astype(jnp.int32)[None]

    slots = range(half)
    chunk = section_inputs.shape[1]
    held_in, held_out = w_in[0], w_out[0]
    received_in = [send(held_in, places.weight_pairs(slot)) for slot in slots]
    received_out = [send(held_out, places.weight_pairs(slot)) for slot in slots]
    everyone = range(places.sections)
    currents = [send(section_inputs[0], places.token_pairs(slot, everyone)) for slot in slots]
    selected = jnp.concatenate(
        [
            lax.dynamic_index_in_dim(patches, plan[tick_index], 0, keepdims=False)
            for tick_index in range(TICKS - 1)
        ],
        axis=0,
    )
    waiting = [send(selected, places.token_pairs(slot, [0])) for slot in slots]

    partner = places.partner_pairs()

    def shared(held, received):
        given = send(held, places.own_pairs(False))
        returned = send(received[0], places.own_pairs(True))
        own, other = [held, returned], [given, received[0]]
        for shard in received[1:]:
            swapped = send(shard, partner)
            own += [shard, swapped]
            other += [swapped, shard]
        return assemble(is_own.astype(jnp.int32)[None], own, other)

    full_in = shared(held_in, received_in)
    small = after(in_bias, *received_in)
    biases = [small] + [
        lax.ppermute(
            small, "tensor", [((place + step) % tensors, place) for place in range(tensors)]
        )
        for step in range(1, tensors)
    ]
    bias = jnp.concatenate(biases, axis=1).astype(jnp.float32)
    rows = after(jnp.concatenate([norm_gain, norm_bias, out_bias], axis=0), *received_in)
    bias = jnp.where(is_own, bias, send(bias, partner))
    rows = jnp.where(is_own, rows, send(rows, partner))
    full_out = shared(held_out, received_out)

    pieces = []
    flag, fresh, first_row = jnp.zeros_like(is_first), currents, 0
    for tick_index in range(TICKS):
        produced = [
            run_block(first_row, flag, currents[slot], fresh[slot], rows, bias, full_in, full_out)
            for slot in slots
        ]
        if tick_index + 1 == TICKS:
            pieces += [send(produced[slot], places.home_pairs(slot, 1)) for slot in slots]
        else:
            currents = [send(produced[slot], places.hop_pairs()) for slot in slots]
            pieces += [send(currents[slot], places.home_pairs(slot, 0)) for slot in slots]
            flag, fresh, first_row = is_first, waiting, tick_index * chunk
    return collect((tensor_index % half)[None], pieces, half)[None]


def gathered(section_inputs, w_in, in_bias, w_out, out_bias, norm_gain, norm_bias, patches, plan):
    sections = lax.axis_size("section")
    section_index = lax.axis_index("section")
    gather = lambda value: lax.all_gather(value, "tensor", axis=0, tiled=True)
    full_in, full_bias, full_out = gather(w_in[0]), gather(in_bias[0]), gather(w_out[0])
    weights = [(full_in, full_bias.astype(jnp.float32), full_out)]
    current = section_inputs[0]
    records = []
    for tick_index in range(TICKS):
        produced = apply_block(current, weights, norm_gain[0], norm_bias[0], out_bias[0])
        pairs = [(source, (source + 1) % sections) for source in range(sections)]
        arrived = lax.ppermute(produced, "section", pairs)
        records.append(arrived)
        if tick_index + 1 < TICKS:
            selected = lax.dynamic_index_in_dim(patches, plan[tick_index], 0, keepdims=False)
            current = jnp.where(section_index == 0, selected, arrived)
    return jnp.stack(records, axis=0)[None]


def solution(mesh):
    sections, tensors = mesh.shape["section"], mesh.shape["tensor"]
    fits = sections % 2 == 0 and tensors % 2 == 0 and tensors <= sections // 2
    placed = (
        P("section", "tensor", None),
        P("section", "tensor", None),
        P("section", "tensor"),
        P("section", "tensor", None),
        P("section", None),
        P("section", None),
        P("section", None),
        P(None, "tensor", None),
        P(),
    )
    return jax.shard_map(
        collapsed if fits else gathered,
        mesh=mesh,
        in_specs=placed,
        out_specs=P("section", None, "tensor", None),
        check_vma=False,
    )
```

```python
import functools

import jax
import jax.numpy as jnp
from jax import lax
from jax.experimental import pallas as pl
from jax.experimental.pallas import tpu as pltpu
from jax.sharding import PartitionSpec as P


TICKS = 4


norm_floor = 0.1
gelu_slope = 1.702


class Plan:
    def __init__(self, sections, tensors):
        self.sections = sections
        self.tensors = tensors
        self.half = tensors // 2

    def side(self, section):
        return (section // 2 + section) % 2

    def stage(self, section):
        return self.half - 1 + self.side(section)

    def device(self, section, tensor):
        return section * self.tensors + tensor

    def worker(self, section, core):
        return self.device(section // 2 * 2 + core, self.stage(section))

    def weight_pairs(self, slot):
        return [
            (
                self.device(section, (self.stage(section) + step) % self.tensors),
                self.worker(section, (section + step) % 2),
            )
            for section in range(self.sections)
            for step in (2 * slot, 2 * slot + 1)
            if step > 0
        ]

    def own_pairs(self, back):
        pairs = [
            (self.worker(section, section % 2), self.worker(section, 1 - section % 2))
            for section in range(self.sections)
        ]
        return [(target, source) for source, target in pairs] if back else pairs

    def token_pairs(self, slot, sections):
        return [
            (self.device(section, core * self.half + slot), self.worker(section, core))
            for section in sections
            for core in range(2)
        ]

    def partner_pairs(self):
        return [
            (self.worker(section, core), self.worker(section, 1 - core))
            for section in range(self.sections)
            for core in range(2)
        ]

    def hop_pairs(self):
        return [
            (self.worker(section, core), self.worker((section + 1) % self.sections, core))
            for section in range(self.sections)
            for core in range(2)
        ]

    def crowded(self, section, tensor):
        return section % 2 == 0 and (tensor >= self.half) != self.side(section)

    def home_pairs(self, slot, shift, crowded=None):
        pairs = []
        for section in range(self.sections):
            for core in range(2):
                tensor = core * self.half + slot
                if crowded is None or self.crowded(section, tensor) == crowded:
                    source = self.worker((section - shift) % self.sections, core)
                    pairs.append((source, self.device(section, tensor)))
        return pairs


def send(value, pairs):
    return lax.ppermute(value, ("section", "tensor"), pairs)


def normalize(current, gain_row, shift_row):
    widened = current.astype(jnp.float32)
    average = jnp.mean(widened, axis=-1, keepdims=True)
    centered = widened - average
    variance = jnp.mean(centered * centered, axis=-1, keepdims=True)
    normed = (centered * lax.rsqrt(variance + norm_floor) * gain_row + shift_row).astype(
        jnp.bfloat16
    )
    return (normed, widened)


def activate(preact):
    return preact * jax.nn.sigmoid(gelu_slope * preact)


def apply_block(current, weights, gain_row, shift_row, bias_row):
    normed, widened = normalize(current, gain_row, shift_row)
    total = None
    for rows_in, rows_bias, rows_out in weights:
        preact = lax.dot_general(
            normed, rows_in, (((1,), (1,)), ((), ())), preferred_element_type=jnp.float32
        )
        hidden = activate(preact + rows_bias).astype(jnp.bfloat16)
        part = jnp.dot(hidden, rows_out, preferred_element_type=jnp.float32)
        total = part if total is None else total + part
    return (widened + total + bias_row).astype(jnp.bfloat16)


OWN, FIRST, CROWDED, SLOT = range(4)


def block_kernel(first_row, n_kept, flags, arrived, fresh, rows, bias, rows_in, rows_out, *refs):
    kept, produced, boxes = refs[:n_kept], refs[n_kept], refs[n_kept + 1 :]
    size = arrived.shape[0]
    if first_row is None:
        current = arrived[...]
    else:
        new = fresh[first_row : first_row + size, :]
        current = jnp.where(flags[FIRST] == 1, new, arrived[...])
    normed, widened = normalize(current, rows[0:1, :], rows[1:2, :])
    preact = lax.dot_general(
        normed, rows_in[...], (((1,), (1,)), ((), ())), preferred_element_type=jnp.float32
    )
    hidden = activate(preact + bias[...]).astype(jnp.bfloat16)
    total = jnp.dot(hidden, rows_out[...], preferred_element_type=jnp.float32)
    result = (widened + total + rows[2:3, :]).astype(jnp.bfloat16)
    produced[...] = result
    if boxes:
        products, arrivals = boxes
        earlier = products.shape[0] // size - 1
        for index in range(earlier):
            products[index * size : (index + 1) * size, :] = kept[index][...]
        products[earlier * size :, :] = result
        for index in range(earlier - 1):
            arrivals[index * size : (index + 1) * size, :] = kept[earlier + index][...]
        arrivals[(earlier - 1) * size :, :] = arrived[...]


def run_block(first_row, flags, arrived, fresh, operands, products=None, arrivals=None):
    vector = pl.BlockSpec(memory_space=pltpu.VMEM)
    chunk = lambda count: jax.ShapeDtypeStruct((count * arrived.shape[0],) + arrived.shape[1:], arrived.dtype)
    shapes, kept = [chunk(1)], []
    if products is not None:
        kept = products + arrivals
        shapes += [chunk(len(products) + 1), chunk(len(arrivals) + 1)]
    return pl.pallas_call(
        functools.partial(block_kernel, first_row, len(kept)),
        out_shape=shapes,
        in_specs=[pl.BlockSpec(memory_space=pltpu.SMEM)] + [vector] * (6 + len(kept)),
        out_specs=[vector] * len(shapes),
        compiler_params=pltpu.CompilerParams(vmem_limit_bytes=8 * 2**20),
        name="section_block",
    )(flags, arrived, fresh, *operands, *kept)


def collect_kernel(slots, flags, *refs):
    records = refs[-1]
    parts = [refs[index * slots : (index + 1) * slots] for index in range(4)]
    from_producer, early, late, final = parts
    size = records.shape[1]
    ticks = records.shape[0]

    def mine(part, start):
        value = part[0][start : start + size, :]
        for slot in range(1, slots):
            value = jnp.where(flags[SLOT] == slot, part[slot][start : start + size, :], value)
        return value

    for tick in range(ticks - 1):
        own = mine(late, 0) if tick == ticks - 2 else mine(early, tick * size)
        records[tick] = jnp.where(flags[CROWDED] == 1, mine(from_producer, tick * size), own)
    records[ticks - 1] = mine(final, 0)


def collect(flags, from_producer, early, late, final):
    vector = pl.BlockSpec(memory_space=pltpu.VMEM)
    pieces = from_producer + early + late + final
    return pl.pallas_call(
        functools.partial(collect_kernel, len(final)),
        out_shape=jax.ShapeDtypeStruct((TICKS,) + final[0].shape, final[0].dtype),
        in_specs=[pl.BlockSpec(memory_space=pltpu.SMEM)] + [vector] * len(pieces),
        out_specs=vector,
        compiler_params=pltpu.CompilerParams(vmem_limit_bytes=8 * 2**20),
        name="collect_quarters",
    )(flags, *pieces)


def assemble_kernel(count, flags, *refs):
    own, other, full, done = refs[:count], refs[count : 2 * count], refs[-2], refs[-1]
    size = own[0].shape[0]

    def place(parts):
        copies = [
            pltpu.make_async_copy(part, full.at[pl.ds(step * size, size)], done.at[step])
            for step, part in enumerate(parts)
        ]
        for copy in copies:
            copy.start()
        for copy in copies:
            copy.wait()

    @pl.when(flags[OWN] == 1)
    def _():
        place(own)

    @pl.when(flags[OWN] == 0)
    def _():
        place(other)


def assemble(flags, own, other):
    main = pl.BlockSpec(memory_space=pltpu.MemorySpace.HBM)
    size, width = own[0].shape
    return pl.pallas_call(
        functools.partial(assemble_kernel, len(own)),
        out_shape=jax.ShapeDtypeStruct((size * len(own), width), own[0].dtype),
        in_specs=[pl.BlockSpec(memory_space=pltpu.SMEM)] + [main] * (2 * len(own)),
        out_specs=pl.BlockSpec(memory_space=pltpu.VMEM),
        scratch_shapes=[pltpu.SemaphoreType.DMA((len(own),))],
        compiler_params=pltpu.CompilerParams(vmem_limit_bytes=8 * 2**20),
        name="assemble_shards",
    )(flags, *own, *other)


def collapsed(section_inputs, w_in, in_bias, w_out, out_bias, norm_gain, norm_bias, patches, plan):
    places = Plan(lax.axis_size("section"), lax.axis_size("tensor"))
    tensors, half = places.tensors, places.half
    section_index = lax.axis_index("section")
    tensor_index = lax.axis_index("tensor")
    core = section_index % 2
    line = section_index // 2
    side = (tensor_index >= half).astype(jnp.int32)
    own_core = (line + side) % 2
    is_own = core == own_core
    is_first = (line == 0) & (own_core == 0)
    is_crowded = (core == 0) & (side != line % 2)
    flags = jnp.stack(
        [flag.astype(jnp.int32) for flag in (is_own, is_first, is_crowded, tensor_index % half)]
    )

    slots = range(half)
    chunk = section_inputs.shape[1]
    everyone = range(places.sections)
    partner = places.partner_pairs()

    def spread(value):
        return [send(value, places.weight_pairs(slot)) for slot in slots]

    def shared(held, received):
        given = send(held, places.own_pairs(False))
        returned = send(received[0], places.own_pairs(True))
        own, other = [held, returned], [given, received[0]]
        for slot in range(1, half):
            swapped = send(received[slot], partner)
            own += [received[slot], swapped]
            other += [swapped, received[slot]]
        return assemble(flags, own, other)

    def tokens(value, sections):
        return [send(value, places.token_pairs(slot, sections)) for slot in slots]

    received_in = spread(w_in[0])
    received_out = spread(w_out[0])
    currents = tokens(section_inputs[0], everyone)
    selected = jnp.concatenate(
        [
            lax.dynamic_index_in_dim(patches, plan[tick_index], 0, keepdims=False)
            for tick_index in range(TICKS - 1)
        ],
        axis=0,
    )
    waiting = tokens(selected, [0])

    biases = [in_bias]
    for step in range(1, tensors):
        pairs = [((place + step) % tensors, place) for place in range(tensors)]
        biases.append(lax.ppermute(in_bias, "tensor", pairs))
    bias = jnp.concatenate(biases, axis=1).astype(jnp.float32)
    rows = jnp.concatenate([norm_gain, norm_bias, out_bias], axis=0)
    bias = jnp.where(is_own, bias, send(bias, partner))
    rows = jnp.where(is_own, rows, send(rows, partner))
    full_in = shared(w_in[0], received_in)
    full_out = shared(w_out[0], received_out)
    operands = (rows, bias, full_in, full_out)

    def home(values, shift, crowded):
        return [send(values[slot], places.home_pairs(slot, shift, crowded)) for slot in slots]

    def hop(values):
        return [send(values[slot], places.hop_pairs()) for slot in slots]

    def block(tick_index, slot, *boxes):
        new = waiting if tick_index else currents
        first_row = (tick_index - 1) * chunk if tick_index else None
        return run_block(first_row, flags, currents[slot], new[slot], operands, *boxes)

    products, arrivals = [[] for _ in slots], [[] for _ in slots]
    for tick_index in range(TICKS - 2):
        for slot in slots:
            products[slot] += block(tick_index, slot)
        currents = hop([made[-1] for made in products])
        for slot in slots:
            arrivals[slot].append(currents[slot])

    boxed = [block(TICKS - 2, slot, products[slot], arrivals[slot][:-1]) for slot in slots]
    currents = hop([box[0] for box in boxed])
    from_producer = home([box[1] for box in boxed], 1, True)
    early = home([box[2] for box in boxed], 0, False)
    late = home(currents, 0, False)
    final = home([block(TICKS - 1, slot)[0] for slot in slots], 1, None)
    return collect(flags, from_producer, early, late, final)[None]


def gathered(section_inputs, w_in, in_bias, w_out, out_bias, norm_gain, norm_bias, patches, plan):
    sections = lax.axis_size("section")
    section_index = lax.axis_index("section")
    gather = lambda value: lax.all_gather(value, "tensor", axis=0, tiled=True)
    full_in, full_bias, full_out = gather(w_in[0]), gather(in_bias[0]), gather(w_out[0])
    weights = [(full_in, full_bias.astype(jnp.float32), full_out)]
    current = section_inputs[0]
    records = []
    for tick_index in range(TICKS):
        produced = apply_block(current, weights, norm_gain[0], norm_bias[0], out_bias[0])
        pairs = [(source, (source + 1) % sections) for source in range(sections)]
        arrived = lax.ppermute(produced, "section", pairs)
        records.append(arrived)
        if tick_index + 1 < TICKS:
            selected = lax.dynamic_index_in_dim(patches, plan[tick_index], 0, keepdims=False)
            current = jnp.where(section_index == 0, selected, arrived)
    return jnp.stack(records, axis=0)[None]


def solution(mesh):
    sections, tensors = mesh.shape["section"], mesh.shape["tensor"]
    fits = sections % 2 == 0 and tensors % 2 == 0 and tensors <= sections // 2
    placed = (
        P("section", "tensor", None),
        P("section", "tensor", None),
        P("section", "tensor"),
        P("section", "tensor", None),
        P("section", None),
        P("section", None),
        P("section", None),
        P(None, "tensor", None),
        P(),
    )

    def body(*args):
        return (collapsed if fits else gathered)(*args)

    return jax.shard_map(
        body,
        mesh=mesh,
        in_specs=placed,
        out_specs=P("section", None, "tensor", None),
        check_vma=False,
    )
```

```python
import functools

import jax
import jax.numpy as jnp
from jax import lax
from jax.experimental import pallas as pl
from jax.experimental.pallas import tpu as pltpu
from jax.sharding import PartitionSpec as P


TICKS = 4


norm_floor = 0.1
gelu_slope = 1.702


class Plan:
    def __init__(self, sections, tensors):
        self.sections = sections
        self.tensors = tensors
        self.half = tensors // 2

    def side(self, section):
        return (section // 2 + section) % 2

    def stage(self, section):
        return self.half - 1 + self.side(section)

    def device(self, section, tensor):
        return section * self.tensors + tensor

    def worker(self, section, core):
        return self.device(section // 2 * 2 + core, self.stage(section))

    def weight_pairs(self, slot):
        return [
            (
                self.device(section, (self.stage(section) + step) % self.tensors),
                self.worker(section, (section + step) % 2),
            )
            for section in range(self.sections)
            for step in (2 * slot, 2 * slot + 1)
            if step > 0
        ]

    def own_pairs(self, back):
        pairs = [
            (self.worker(section, section % 2), self.worker(section, 1 - section % 2))
            for section in range(self.sections)
        ]
        return [(target, source) for source, target in pairs] if back else pairs

    def token_pairs(self, slot, sections):
        return [
            (self.device(section, core * self.half + slot), self.worker(section, core))
            for section in sections
            for core in range(2)
        ]

    def partner_pairs(self):
        return [
            (self.worker(section, core), self.worker(section, 1 - core))
            for section in range(self.sections)
            for core in range(2)
        ]

    def hop_pairs(self):
        return [
            (self.worker(section, core), self.worker((section + 1) % self.sections, core))
            for section in range(self.sections)
            for core in range(2)
        ]

    def kept_near(self, section, tensor):
        return section % 2 == 1 and (tensor >= self.half) == self.side(section)

    def home_pairs(self, slot, shift, near=None):
        pairs = []
        for section in range(self.sections):
            for core in range(2):
                tensor = core * self.half + slot
                if near is None or self.kept_near(section, tensor) == near:
                    source = self.worker((section - shift) % self.sections, core)
                    pairs.append((source, self.device(section, tensor)))
        return pairs


def send(value, pairs):
    return lax.ppermute(value, ("section", "tensor"), pairs)


def normalize(current, gain_row, shift_row):
    widened = current.astype(jnp.float32)
    average = jnp.mean(widened, axis=-1, keepdims=True)
    centered = widened - average
    variance = jnp.mean(centered * centered, axis=-1, keepdims=True)
    normed = (centered * lax.rsqrt(variance + norm_floor) * gain_row + shift_row).astype(
        jnp.bfloat16
    )
    return (normed, widened)


def activate(preact):
    return preact * jax.nn.sigmoid(gelu_slope * preact)


def apply_block(current, weights, gain_row, shift_row, bias_row):
    normed, widened = normalize(current, gain_row, shift_row)
    total = None
    for rows_in, rows_bias, rows_out in weights:
        preact = lax.dot_general(
            normed, rows_in, (((1,), (1,)), ((), ())), preferred_element_type=jnp.float32
        )
        hidden = activate(preact + rows_bias).astype(jnp.bfloat16)
        part = jnp.dot(hidden, rows_out, preferred_element_type=jnp.float32)
        total = part if total is None else total + part
    return (widened + total + bias_row).astype(jnp.bfloat16)


OWN, FIRST, NEAR, SLOT = range(4)


def block_kernel(first_row, n_kept, box_products, flags, arrived, fresh, rows, bias, rows_in, rows_out, *refs):
    kept, produced, boxes = refs[:n_kept], refs[n_kept], refs[n_kept + 1 :]
    size = arrived.shape[0]
    if first_row is None:
        current = arrived[...]
    else:
        new = fresh[first_row : first_row + size, :]
        current = jnp.where(flags[FIRST] == 1, new, arrived[...])
    normed, widened = normalize(current, rows[0:1, :], rows[1:2, :])
    preact = lax.dot_general(
        normed, rows_in[...], (((1,), (1,)), ((), ())), preferred_element_type=jnp.float32
    )
    hidden = activate(preact + bias[...]).astype(jnp.bfloat16)
    total = jnp.dot(hidden, rows_out[...], preferred_element_type=jnp.float32)
    result = (widened + total + rows[2:3, :]).astype(jnp.bfloat16)
    produced[...] = result
    if boxes:
        for index in range(n_kept):
            boxes[0][index * size : (index + 1) * size, :] = kept[index][...]
        boxes[0][n_kept * size :, :] = result if box_products else arrived[...]


def run_block(first_row, flags, arrived, fresh, operands, kept=(), box_products=False):
    vector = pl.BlockSpec(memory_space=pltpu.VMEM)
    size, width = arrived.shape
    shapes = [jax.ShapeDtypeStruct((size, width), arrived.dtype)]
    if kept:
        shapes.append(jax.ShapeDtypeStruct(((len(kept) + 1) * size, width), arrived.dtype))
    return pl.pallas_call(
        functools.partial(block_kernel, first_row, len(kept), box_products),
        out_shape=shapes,
        in_specs=[pl.BlockSpec(memory_space=pltpu.SMEM)] + [vector] * (6 + len(kept)),
        out_specs=[vector] * len(shapes),
        compiler_params=pltpu.CompilerParams(vmem_limit_bytes=8 * 2**20),
        name="section_block",
    )(flags, arrived, fresh, *operands, *kept)


def collect_kernel(slots, flags, *refs):
    records = refs[-1]
    parts = [refs[index * slots : (index + 1) * slots] for index in range(4)]
    near, early, late, final = parts
    size = records.shape[1]
    ticks = records.shape[0]

    def mine(part, start):
        value = part[0][start : start + size, :]
        for slot in range(1, slots):
            value = jnp.where(flags[SLOT] == slot, part[slot][start : start + size, :], value)
        return value

    for tick in range(ticks - 2):
        start = tick * size
        records[tick] = jnp.where(flags[NEAR] == 1, mine(near, start), mine(early, start))
    records[ticks - 2] = mine(late, 0)
    records[ticks - 1] = mine(final, 0)


def collect(flags, near, early, late, final):
    vector = pl.BlockSpec(memory_space=pltpu.VMEM)
    pieces = near + early + late + final
    return pl.pallas_call(
        functools.partial(collect_kernel, len(final)),
        out_shape=jax.ShapeDtypeStruct((TICKS,) + final[0].shape, final[0].dtype),
        in_specs=[pl.BlockSpec(memory_space=pltpu.SMEM)] + [vector] * len(pieces),
        out_specs=vector,
        compiler_params=pltpu.CompilerParams(vmem_limit_bytes=8 * 2**20),
        name="collect_quarters",
    )(flags, *pieces)


def assemble_kernel(count, flags, *refs):
    own, other, full, done = refs[:count], refs[count : 2 * count], refs[-2], refs[-1]
    size = own[0].shape[0]

    def place(parts):
        copies = [
            pltpu.make_async_copy(part, full.at[pl.ds(step * size, size)], done.at[step])
            for step, part in enumerate(parts)
        ]
        for copy in copies:
            copy.start()
        for copy in copies:
            copy.wait()

    @pl.when(flags[OWN] == 1)
    def _():
        place(own)

    @pl.when(flags[OWN] == 0)
    def _():
        place(other)


def assemble(flags, own, other):
    main = pl.BlockSpec(memory_space=pltpu.MemorySpace.HBM)
    size, width = own[0].shape
    return pl.pallas_call(
        functools.partial(assemble_kernel, len(own)),
        out_shape=jax.ShapeDtypeStruct((size * len(own), width), own[0].dtype),
        in_specs=[pl.BlockSpec(memory_space=pltpu.SMEM)] + [main] * (2 * len(own)),
        out_specs=pl.BlockSpec(memory_space=pltpu.VMEM),
        scratch_shapes=[pltpu.SemaphoreType.DMA((len(own),))],
        compiler_params=pltpu.CompilerParams(vmem_limit_bytes=8 * 2**20),
        name="assemble_shards",
    )(flags, *own, *other)


def collapsed(section_inputs, w_in, in_bias, w_out, out_bias, norm_gain, norm_bias, patches, plan):
    places = Plan(lax.axis_size("section"), lax.axis_size("tensor"))
    tensors, half = places.tensors, places.half
    section_index = lax.axis_index("section")
    tensor_index = lax.axis_index("tensor")
    core = section_index % 2
    line = section_index // 2
    side = (tensor_index >= half).astype(jnp.int32)
    own_core = (line + side) % 2
    is_own = core == own_core
    is_first = (line == 0) & (own_core == 0)
    is_near = (core == 1) & (side != line % 2)
    flags = jnp.stack(
        [flag.astype(jnp.int32) for flag in (is_own, is_first, is_near, tensor_index % half)]
    )

    slots = range(half)
    chunk = section_inputs.shape[1]
    everyone = range(places.sections)
    partner = places.partner_pairs()

    def spread(value):
        return [send(value, places.weight_pairs(slot)) for slot in slots]

    def shared(held, received):
        given = send(held, places.own_pairs(False))
        returned = send(received[0], places.own_pairs(True))
        own, other = [held, returned], [given, received[0]]
        for slot in range(1, half):
            swapped = send(received[slot], partner)
            own += [received[slot], swapped]
            other += [swapped, received[slot]]
        return assemble(flags, own, other)

    def tokens(value, sections):
        return [send(value, places.token_pairs(slot, sections)) for slot in slots]

    received_in = spread(w_in[0])
    received_out = spread(w_out[0])
    currents = tokens(section_inputs[0], everyone)
    selected = jnp.concatenate(
        [
            lax.dynamic_index_in_dim(patches, plan[tick_index], 0, keepdims=False)
            for tick_index in range(TICKS - 1)
        ],
        axis=0,
    )
    waiting = tokens(selected, [0])

    biases = [in_bias]
    for step in range(1, tensors):
        pairs = [((place + step) % tensors, place) for place in range(tensors)]
        biases.append(lax.ppermute(in_bias, "tensor", pairs))
    bias = jnp.concatenate(biases, axis=1).astype(jnp.float32)
    rows = jnp.concatenate([norm_gain, norm_bias, out_bias], axis=0)
    bias = jnp.where(is_own, bias, send(bias, partner))
    rows = jnp.where(is_own, rows, send(rows, partner))
    full_in = shared(w_in[0], received_in)
    full_out = shared(w_out[0], received_out)
    operands = (rows, bias, full_in, full_out)

    def home(values, shift, near):
        return [send(values[slot], places.home_pairs(slot, shift, near)) for slot in slots]

    def hop(values):
        return [send(values[slot], places.hop_pairs()) for slot in slots]

    def blocks(tick_index, *boxes):
        new = waiting if tick_index else currents
        first_row = (tick_index - 1) * chunk if tick_index else None
        made = []
        for slot in slots:
            kept = [boxes[0][slot]] if boxes else []
            made.append(
                run_block(first_row, flags, currents[slot], new[slot], operands, kept, *boxes[1:])
            )
        return list(zip(*made))

    (products,) = blocks(0)
    currents = hop(products)
    arrivals = currents
    products, boxed = blocks(1, products, True)
    currents = hop(products)
    early = home(boxed, 1, False)
    products, boxed = blocks(2, arrivals, False)
    currents = hop(products)
    late = home(products, 1, None)
    near = home(boxed, 0, True)
    (products,) = blocks(3)
    final = home(products, 1, None)
    return collect(flags, near, early, late, final)[None]


def gathered(section_inputs, w_in, in_bias, w_out, out_bias, norm_gain, norm_bias, patches, plan):
    sections = lax.axis_size("section")
    section_index = lax.axis_index("section")
    gather = lambda value: lax.all_gather(value, "tensor", axis=0, tiled=True)
    full_in, full_bias, full_out = gather(w_in[0]), gather(in_bias[0]), gather(w_out[0])
    weights = [(full_in, full_bias.astype(jnp.float32), full_out)]
    current = section_inputs[0]
    records = []
    for tick_index in range(TICKS):
        produced = apply_block(current, weights, norm_gain[0], norm_bias[0], out_bias[0])
        pairs = [(source, (source + 1) % sections) for source in range(sections)]
        arrived = lax.ppermute(produced, "section", pairs)
        records.append(arrived)
        if tick_index + 1 < TICKS:
            selected = lax.dynamic_index_in_dim(patches, plan[tick_index], 0, keepdims=False)
            current = jnp.where(section_index == 0, selected, arrived)
    return jnp.stack(records, axis=0)[None]


def solution(mesh):
    sections, tensors = mesh.shape["section"], mesh.shape["tensor"]
    fits = sections % 2 == 0 and tensors % 2 == 0 and tensors <= sections // 2
    placed = (
        P("section", "tensor", None),
        P("section", "tensor", None),
        P("section", "tensor"),
        P("section", "tensor", None),
        P("section", None),
        P("section", None),
        P("section", None),
        P(None, "tensor", None),
        P(),
    )

    def body(*args):
        return (collapsed if fits else gathered)(*args)

    return jax.shard_map(
        body,
        mesh=mesh,
        in_specs=placed,
        out_specs=P("section", None, "tensor", None),
        check_vma=False,
    )
```

```python
import functools

import jax
import jax.numpy as jnp
from jax import lax
from jax.experimental import pallas as pl
from jax.experimental.pallas import tpu as pltpu
from jax.sharding import PartitionSpec as P


TICKS = 4


norm_floor = 0.1
gelu_slope = 1.702


class Plan:
    def __init__(self, sections, tensors):
        self.sections = sections
        self.tensors = tensors
        self.half = tensors // 2

    def side(self, section):
        return (section // 2 + section) % 2

    def stage(self, section):
        return self.half - 1 + self.side(section)

    def device(self, section, tensor):
        return section * self.tensors + tensor

    def worker(self, section, core):
        return self.device(section // 2 * 2 + core, self.stage(section))

    def weight_pairs(self, slot):
        return [
            (
                self.device(section, (self.stage(section) + step) % self.tensors),
                self.worker(section, (section + step) % 2),
            )
            for section in range(self.sections)
            for step in (2 * slot, 2 * slot + 1)
            if step > 0
        ]

    def own_pairs(self, back):
        pairs = [
            (self.worker(section, section % 2), self.worker(section, 1 - section % 2))
            for section in range(self.sections)
        ]
        return [(target, source) for source, target in pairs] if back else pairs

    def quarter(self, core, slot):
        return self.tensors - 1 - slot if core else slot

    def token_pairs(self, slot, sections):
        return [
            (self.device(section, self.quarter(core, slot)), self.worker(section, core))
            for section in sections
            for core in range(2)
        ]

    def partner_pairs(self):
        return [
            (self.worker(section, core), self.worker(section, 1 - core))
            for section in range(self.sections)
            for core in range(2)
        ]

    def hop_pairs(self):
        return [
            (self.worker(section, core), self.worker((section + 1) % self.sections, core))
            for section in range(self.sections)
            for core in range(2)
        ]

    def kept_near(self, section, tensor):
        return section % 2 == 1 and (tensor >= self.half) == self.side(section)

    def home_pairs(self, slot, shift, near=None):
        pairs = []
        for section in range(self.sections):
            for core in range(2):
                tensor = self.quarter(core, slot)
                if near is None or self.kept_near(section, tensor) == near:
                    source = self.worker((section - shift) % self.sections, core)
                    pairs.append((source, self.device(section, tensor)))
        return pairs


    def marks(self):
        table = []
        for section in range(self.sections):
            for tensor in range(self.tensors):
                side = int(tensor >= self.half)
                own = (section // 2 + side) % 2
                slot = self.tensors - 1 - tensor if side else tensor
                first = section < 2 and own == 0
                near = self.kept_near(section, tensor)
                table.append([float(mark) for mark in (section % 2 == own, first, near, slot)])
        return table


def send(value, pairs):
    return lax.ppermute(value, ("section", "tensor"), pairs)


def normalize(current, gain_row, shift_row):
    widened = current.astype(jnp.float32)
    average = jnp.mean(widened, axis=-1, keepdims=True)
    centered = widened - average
    variance = jnp.mean(centered * centered, axis=-1, keepdims=True)
    normed = (centered * lax.rsqrt(variance + norm_floor) * gain_row + shift_row).astype(
        jnp.bfloat16
    )
    return (normed, widened)


def activate(preact):
    return preact * jax.nn.sigmoid(gelu_slope * preact)


def apply_block(current, weights, gain_row, shift_row, bias_row):
    normed, widened = normalize(current, gain_row, shift_row)
    total = None
    for rows_in, rows_bias, rows_out in weights:
        preact = lax.dot_general(
            normed, rows_in, (((1,), (1,)), ((), ())), preferred_element_type=jnp.float32
        )
        hidden = activate(preact + rows_bias).astype(jnp.bfloat16)
        part = jnp.dot(hidden, rows_out, preferred_element_type=jnp.float32)
        total = part if total is None else total + part
    return (widened + total + bias_row).astype(jnp.bfloat16)


GAIN, SHIFT, BIAS, OWN, FIRST, NEAR, SLOT = range(7)


def row(rows, index):
    return rows[index : index + 1, :]


def mark(rows, index):
    return jnp.max(row(rows, index))


def enter_kernel(arrived, rows, bias, rows_in, hidden):
    normed, _ = normalize(arrived[...], row(rows, GAIN), row(rows, SHIFT))
    preact = lax.dot_general(
        normed, rows_in[...], (((1,), (1,)), ((), ())), preferred_element_type=jnp.float32
    )
    hidden[...] = activate(preact + bias[...]).astype(jnp.bfloat16)


def leave_kernel(arrived, hidden, rows, rows_out, produced):
    total = jnp.dot(hidden[...], rows_out[...], preferred_element_type=jnp.float32)
    widened = arrived[...].astype(jnp.float32)
    produced[...] = (widened + total + row(rows, BIAS)).astype(jnp.bfloat16)


def enter(arrived, rows, bias, full_in):
    vector = pl.BlockSpec(memory_space=pltpu.VMEM)
    return pl.pallas_call(
        enter_kernel,
        out_shape=jax.ShapeDtypeStruct((arrived.shape[0], full_in.shape[0]), jnp.bfloat16),
        in_specs=[vector] * 4,
        out_specs=vector,
        compiler_params=pltpu.CompilerParams(vmem_limit_bytes=8 * 2**20),
        name="enter_block",
    )(arrived, rows, bias, full_in)


def leave(arrived, hidden, rows, full_out):
    vector = pl.BlockSpec(memory_space=pltpu.VMEM)
    return pl.pallas_call(
        leave_kernel,
        out_shape=jax.ShapeDtypeStruct(arrived.shape, arrived.dtype),
        in_specs=[vector] * 4,
        out_specs=vector,
        compiler_params=pltpu.CompilerParams(vmem_limit_bytes=8 * 2**20),
        name="leave_block",
    )(arrived, hidden, rows, full_out)


def block_kernel(
    first_row, n_kept, box_products, arrived, fresh, rows, bias, rows_in, rows_out, *refs
):
    kept, produced, boxes = refs[:n_kept], refs[n_kept], refs[n_kept + 1 :]
    size = arrived.shape[0]
    new = fresh[first_row : first_row + size, :].astype(jnp.float32)
    current = jnp.where(row(rows, FIRST) == 1.0, new, arrived[...].astype(jnp.float32))
    normed, widened = normalize(current, row(rows, GAIN), row(rows, SHIFT))
    preact = lax.dot_general(
        normed, rows_in[...], (((1,), (1,)), ((), ())), preferred_element_type=jnp.float32
    )
    hidden = activate(preact + bias[...]).astype(jnp.bfloat16)
    total = jnp.dot(hidden, rows_out[...], preferred_element_type=jnp.float32)
    result = (widened + total + row(rows, BIAS)).astype(jnp.bfloat16)
    produced[...] = result
    if boxes:
        for index in range(n_kept):
            boxes[0][index * size : (index + 1) * size, :] = kept[index][...]
        boxes[0][n_kept * size :, :] = result if box_products else arrived[...]


def run_block(first_row, arrived, fresh, operands, kept=(), box_products=False):
    vector = pl.BlockSpec(memory_space=pltpu.VMEM)
    size, width = arrived.shape
    shapes = [jax.ShapeDtypeStruct((size, width), arrived.dtype)]
    if kept:
        shapes.append(jax.ShapeDtypeStruct(((len(kept) + 1) * size, width), arrived.dtype))
    return pl.pallas_call(
        functools.partial(block_kernel, first_row, len(kept), box_products),
        out_shape=shapes,
        in_specs=[vector] * (6 + len(kept)),
        out_specs=[vector] * len(shapes),
        compiler_params=pltpu.CompilerParams(vmem_limit_bytes=8 * 2**20),
        name="section_block",
    )(arrived, fresh, *operands, *kept)


def collect_kernel(slots, rows, *refs):
    records = refs[-1]
    parts = [refs[index * slots : (index + 1) * slots] for index in range(4)]
    near, early, late, final = parts
    size = records.shape[1]
    ticks = records.shape[0]
    choice, is_near = mark(rows, SLOT), mark(rows, NEAR)

    def mine(part, start):
        value = part[0][start : start + size, :]
        for slot in range(1, slots):
            value = jnp.where(choice == slot, part[slot][start : start + size, :], value)
        return value

    for tick in range(ticks - 2):
        start = tick * size
        records[tick] = jnp.where(is_near == 1.0, mine(near, start), mine(early, start))
    records[ticks - 2] = mine(late, 0)
    records[ticks - 1] = mine(final, 0)


def collect(rows, near, early, late, final):
    vector = pl.BlockSpec(memory_space=pltpu.VMEM)
    pieces = near + early + late + final
    return pl.pallas_call(
        functools.partial(collect_kernel, len(final)),
        out_shape=jax.ShapeDtypeStruct((TICKS,) + final[0].shape, final[0].dtype),
        in_specs=[vector] * (1 + len(pieces)),
        out_specs=vector,
        compiler_params=pltpu.CompilerParams(vmem_limit_bytes=8 * 2**20),
        name="collect_quarters",
    )(rows, *pieces)


def assemble_kernel(count, rows, *refs):
    own, other, full, done = refs[:count], refs[count : 2 * count], refs[-2], refs[-1]
    size = own[0].shape[0]

    def place(parts):
        copies = [
            pltpu.make_async_copy(part, full.at[pl.ds(step * size, size)], done.at[step])
            for step, part in enumerate(parts)
        ]
        for copy in copies:
            copy.start()
        for copy in copies:
            copy.wait()

    is_own = mark(rows, OWN)

    @pl.when(is_own == 1.0)
    def _():
        place(own)

    @pl.when(is_own != 1.0)
    def _():
        place(other)


def assemble(rows, own, other):
    vector = pl.BlockSpec(memory_space=pltpu.VMEM)
    main = pl.BlockSpec(memory_space=pltpu.MemorySpace.HBM)
    size, width = own[0].shape
    return pl.pallas_call(
        functools.partial(assemble_kernel, len(own)),
        out_shape=jax.ShapeDtypeStruct((size * len(own), width), own[0].dtype),
        in_specs=[vector] + [main] * (2 * len(own)),
        out_specs=vector,
        scratch_shapes=[pltpu.SemaphoreType.DMA((len(own),))],
        compiler_params=pltpu.CompilerParams(vmem_limit_bytes=8 * 2**20),
        name="assemble_shards",
    )(rows, *own, *other)


def collapsed(section_inputs, w_in, in_bias, w_out, out_bias, norm_gain, norm_bias, patches, plan):
    places = Plan(lax.axis_size("section"), lax.axis_size("tensor"))
    tensors, half = places.tensors, places.half
    place = lax.axis_index("section") * tensors + lax.axis_index("tensor")
    marks = lax.dynamic_slice_in_dim(jnp.array(places.marks(), jnp.float32), place, 1, 0)
    marks = jnp.broadcast_to(marks[0][:, None], (marks.shape[1], norm_gain.shape[1]))
    is_own = marks[0, 0] == 1.0

    slots = range(half)
    chunk = section_inputs.shape[1]
    everyone = range(places.sections)
    partner = places.partner_pairs()

    def spread(value):
        return [send(value, places.weight_pairs(slot)) for slot in slots]

    def shared(held, received):
        given = send(held, places.own_pairs(False))
        returned = send(received[0], places.own_pairs(True))
        own, other = [held, returned], [given, received[0]]
        for slot in range(1, half):
            swapped = send(received[slot], partner)
            own += [received[slot], swapped]
            other += [swapped, received[slot]]
        return assemble(rows, own, other)

    def tokens(value, sections):
        return [send(value, places.token_pairs(slot, sections)) for slot in slots]

    received_in = spread(w_in[0])
    received_out = spread(w_out[0])
    currents = tokens(section_inputs[0], everyone)
    selected = jnp.concatenate(
        [
            lax.dynamic_index_in_dim(patches, plan[tick_index], 0, keepdims=False)
            for tick_index in range(TICKS - 1)
        ],
        axis=0,
    )
    waiting = tokens(selected, [0])

    biases = [in_bias]
    for step in range(1, tensors):
        pairs = [((to + step) % tensors, to) for to in range(tensors)]
        biases.append(lax.ppermute(in_bias, "tensor", pairs))
    bias = jnp.concatenate(biases, axis=1).astype(jnp.float32)
    rows = jnp.concatenate([norm_gain, norm_bias, out_bias], axis=0)
    bias = jnp.where(is_own, bias, send(bias, partner))
    rows = jnp.where(is_own, rows, send(rows, partner))
    rows = jnp.concatenate([rows, marks], axis=0)
    full_in = shared(w_in[0], received_in)
    hiddens = [enter(currents[slot], rows, bias, full_in) for slot in slots]
    full_out = shared(w_out[0], received_out)
    operands = (rows, bias, full_in, full_out)

    def home(values, shift, near):
        return [send(values[slot], places.home_pairs(slot, shift, near)) for slot in slots]

    def hop(values):
        return [send(values[slot], places.hop_pairs()) for slot in slots]

    def blocks(tick_index, *boxes):
        first_row = (tick_index - 1) * chunk
        made = []
        for slot in slots:
            kept = [boxes[0][slot]] if boxes else []
            made.append(
                run_block(first_row, currents[slot], waiting[slot], operands, kept, *boxes[1:])
            )
        return list(zip(*made))

    products = [leave(currents[slot], hiddens[slot], rows, full_out) for slot in slots]
    currents = hop(products)
    arrivals = currents
    products, boxed = blocks(1, products, True)
    currents = hop(products)
    early = home(boxed, 1, False)
    products, boxed = blocks(2, arrivals, False)
    currents = hop(products)
    late = home(products, 1, None)
    near = home(boxed, 0, True)
    (products,) = blocks(3)
    final = home(products, 1, None)
    return collect(rows, near, early, late, final)[None]


def gathered(section_inputs, w_in, in_bias, w_out, out_bias, norm_gain, norm_bias, patches, plan):
    sections = lax.axis_size("section")
    section_index = lax.axis_index("section")
    gather = lambda value: lax.all_gather(value, "tensor", axis=0, tiled=True)
    full_in, full_bias, full_out = gather(w_in[0]), gather(in_bias[0]), gather(w_out[0])
    weights = [(full_in, full_bias.astype(jnp.float32), full_out)]
    current = section_inputs[0]
    records = []
    for tick_index in range(TICKS):
        produced = apply_block(current, weights, norm_gain[0], norm_bias[0], out_bias[0])
        pairs = [(source, (source + 1) % sections) for source in range(sections)]
        arrived = lax.ppermute(produced, "section", pairs)
        records.append(arrived)
        if tick_index + 1 < TICKS:
            selected = lax.dynamic_index_in_dim(patches, plan[tick_index], 0, keepdims=False)
            current = jnp.where(section_index == 0, selected, arrived)
    return jnp.stack(records, axis=0)[None]


def solution(mesh):
    sections, tensors = mesh.shape["section"], mesh.shape["tensor"]
    fits = sections % 2 == 0 and tensors % 2 == 0 and tensors <= sections // 2
    placed = (
        P("section", "tensor", None),
        P("section", "tensor", None),
        P("section", "tensor"),
        P("section", "tensor", None),
        P("section", None),
        P("section", None),
        P("section", None),
        P(None, "tensor", None),
        P(),
    )

    def body(*args):
        return (collapsed if fits else gathered)(*args)

    return jax.shard_map(
        body,
        mesh=mesh,
        in_specs=placed,
        out_specs=P("section", None, "tensor", None),
        check_vma=False,
    )
```

```python
import functools

import jax
import jax.numpy as jnp
from jax import lax
from jax.experimental import pallas as pl
from jax.experimental.pallas import tpu as pltpu
from jax.sharding import PartitionSpec as P


TICKS = 4


norm_floor = 0.1
gelu_slope = 1.702


class Plan:
    def __init__(self, sections, tensors):
        self.sections = sections
        self.tensors = tensors
        self.half = tensors // 2

    def side(self, section):
        return (section // 2 + section) % 2

    def stage(self, section):
        return self.half - 1 + self.side(section)

    def device(self, section, tensor):
        return section * self.tensors + tensor

    def worker(self, section, core):
        return self.device(section // 2 * 2 + core, self.stage(section))

    def weight_pairs(self, slot):
        return [
            (
                self.device(section, (self.stage(section) + step) % self.tensors),
                self.worker(section, (section + step) % 2),
            )
            for section in range(self.sections)
            for step in (2 * slot, 2 * slot + 1)
            if step > 0
        ]

    def own_pairs(self, back):
        pairs = [
            (self.worker(section, section % 2), self.worker(section, 1 - section % 2))
            for section in range(self.sections)
        ]
        return [(target, source) for source, target in pairs] if back else pairs

    def quarter(self, core, slot):
        return self.tensors - 1 - slot if core else slot

    def token_pairs(self, slot, sections):
        return [
            (self.device(section, self.quarter(core, slot)), self.worker(section, core))
            for section in sections
            for core in range(2)
        ]

    def partner_pairs(self):
        return [
            (self.worker(section, core), self.worker(section, 1 - core))
            for section in range(self.sections)
            for core in range(2)
        ]

    def hop_pairs(self):
        return [
            (self.worker(section, core), self.worker((section + 1) % self.sections, core))
            for section in range(self.sections)
            for core in range(2)
        ]

    def kept_near(self, section, tensor):
        return section % 2 == 1 and (tensor >= self.half) == self.side(section)

    def home_pairs(self, slot, shift, near=None):
        pairs = []
        for section in range(self.sections):
            for core in range(2):
                tensor = self.quarter(core, slot)
                if near is None or self.kept_near(section, tensor) == near:
                    source = self.worker((section - shift) % self.sections, core)
                    pairs.append((source, self.device(section, tensor)))
        return pairs


    def marks(self):
        table = []
        for section in range(self.sections):
            for tensor in range(self.tensors):
                side = int(tensor >= self.half)
                own = (section // 2 + side) % 2
                slot = self.tensors - 1 - tensor if side else tensor
                first = section < 2 and own == 0
                near = self.kept_near(section, tensor)
                table.append([float(mark) for mark in (section % 2 == own, first, near, slot)])
        return table


def send(value, pairs):
    return lax.ppermute(value, ("section", "tensor"), pairs)


def normalize(current, gain_row, shift_row):
    widened = current.astype(jnp.float32)
    average = jnp.mean(widened, axis=-1, keepdims=True)
    centered = widened - average
    variance = jnp.mean(centered * centered, axis=-1, keepdims=True)
    normed = (centered * lax.rsqrt(variance + norm_floor) * gain_row + shift_row).astype(
        jnp.bfloat16
    )
    return (normed, widened)


def activate(preact):
    return preact * jax.nn.sigmoid(gelu_slope * preact)


def apply_block(current, weights, gain_row, shift_row, bias_row):
    normed, widened = normalize(current, gain_row, shift_row)
    total = None
    for rows_in, rows_bias, rows_out in weights:
        preact = lax.dot_general(
            normed, rows_in, (((1,), (1,)), ((), ())), preferred_element_type=jnp.float32
        )
        hidden = activate(preact + rows_bias).astype(jnp.bfloat16)
        part = jnp.dot(hidden, rows_out, preferred_element_type=jnp.float32)
        total = part if total is None else total + part
    return (widened + total + bias_row).astype(jnp.bfloat16)


GAIN, SHIFT, BIAS, OWN, FIRST, NEAR, SLOT = range(7)


def row(rows, index):
    return rows[index : index + 1, :]


def mark(rows, index):
    return jnp.max(row(rows, index))


def enter_kernel(arrived, rows, bias, rows_in, hidden):
    normed, _ = normalize(arrived[...], row(rows, GAIN), row(rows, SHIFT))
    preact = lax.dot_general(
        normed, rows_in[...], (((1,), (1,)), ((), ())), preferred_element_type=jnp.float32
    )
    hidden[...] = activate(preact + bias[...]).astype(jnp.bfloat16)


def leave_kernel(arrived, hidden, rows, rows_out, produced):
    total = jnp.dot(hidden[...], rows_out[...], preferred_element_type=jnp.float32)
    widened = arrived[...].astype(jnp.float32)
    produced[...] = (widened + total + row(rows, BIAS)).astype(jnp.bfloat16)


def enter(arrived, rows, bias, full_in):
    vector = pl.BlockSpec(memory_space=pltpu.VMEM)
    return pl.pallas_call(
        enter_kernel,
        out_shape=jax.ShapeDtypeStruct((arrived.shape[0], full_in.shape[0]), jnp.bfloat16),
        in_specs=[vector] * 4,
        out_specs=vector,
        compiler_params=pltpu.CompilerParams(vmem_limit_bytes=8 * 2**20),
        name="enter_block",
    )(arrived, rows, bias, full_in)


def leave(arrived, hidden, rows, full_out):
    vector = pl.BlockSpec(memory_space=pltpu.VMEM)
    return pl.pallas_call(
        leave_kernel,
        out_shape=jax.ShapeDtypeStruct(arrived.shape, arrived.dtype),
        in_specs=[vector] * 4,
        out_specs=vector,
        compiler_params=pltpu.CompilerParams(vmem_limit_bytes=8 * 2**20),
        name="leave_block",
    )(arrived, hidden, rows, full_out)


def block_kernel(first_row, arrived, fresh, rows, bias, rows_in, rows_out, *refs):
    size = arrived.shape[0]
    new = fresh[first_row : first_row + size, :].astype(jnp.float32)
    current = jnp.where(row(rows, FIRST) == 1.0, new, arrived[...].astype(jnp.float32))
    normed, widened = normalize(current, row(rows, GAIN), row(rows, SHIFT))
    preact = lax.dot_general(
        normed, rows_in[...], (((1,), (1,)), ((), ())), preferred_element_type=jnp.float32
    )
    hidden = activate(preact + bias[...]).astype(jnp.bfloat16)
    total = jnp.dot(hidden, rows_out[...], preferred_element_type=jnp.float32)
    result = (widened + total + row(rows, BIAS)).astype(jnp.bfloat16)
    if len(refs) == 1:
        refs[0][...] = result
        return
    product, arrival, produced, products, arrivals = refs
    produced[...] = result
    products[:size, :] = product[...]
    products[size:, :] = result
    arrivals[:size, :] = arrival[...]
    arrivals[size:, :] = arrived[...]


def run_block(first_row, arrived, fresh, operands, kept=()):
    vector = pl.BlockSpec(memory_space=pltpu.VMEM)
    size, width = arrived.shape
    chunks = [1, 2, 2] if kept else [1]
    shapes = [jax.ShapeDtypeStruct((count * size, width), arrived.dtype) for count in chunks]
    return pl.pallas_call(
        functools.partial(block_kernel, first_row),
        out_shape=shapes,
        in_specs=[vector] * (6 + len(kept)),
        out_specs=[vector] * len(shapes),
        compiler_params=pltpu.CompilerParams(vmem_limit_bytes=8 * 2**20),
        name="section_block",
    )(arrived, fresh, *operands, *kept)


def collect_kernel(slots, rows, *refs):
    records = refs[-1]
    parts = [refs[index * slots : (index + 1) * slots] for index in range(5)]
    early, late, near, near_late, final = parts
    size = records.shape[1]
    ticks = records.shape[0]
    choice, is_near = mark(rows, SLOT), mark(rows, NEAR)

    def mine(part, start):
        value = part[0][start : start + size, :]
        for slot in range(1, slots):
            value = jnp.where(choice == slot, part[slot][start : start + size, :], value)
        return value

    def either(tick, far, far_start, close, close_start):
        records[tick] = jnp.where(is_near == 1.0, mine(close, close_start), mine(far, far_start))

    either(0, early, 0, near, 0)
    either(1, late, 0, near, size)
    either(2, late, size, near_late, 0)
    records[ticks - 1] = mine(final, 0)


def collect(rows, early, late, near, near_late, final):
    vector = pl.BlockSpec(memory_space=pltpu.VMEM)
    pieces = early + late + near + near_late + final
    return pl.pallas_call(
        functools.partial(collect_kernel, len(final)),
        out_shape=jax.ShapeDtypeStruct((TICKS,) + final[0].shape, final[0].dtype),
        in_specs=[vector] * (1 + len(pieces)),
        out_specs=vector,
        compiler_params=pltpu.CompilerParams(vmem_limit_bytes=8 * 2**20),
        name="collect_quarters",
    )(rows, *pieces)


def assemble_kernel(count, rows, *refs):
    own, other, full, done = refs[:count], refs[count : 2 * count], refs[-2], refs[-1]
    size = own[0].shape[0]

    def place(parts):
        copies = [
            pltpu.make_async_copy(part, full.at[pl.ds(step * size, size)], done.at[step])
            for step, part in enumerate(parts)
        ]
        for copy in copies:
            copy.start()
        for copy in copies:
            copy.wait()

    is_own = mark(rows, OWN)

    @pl.when(is_own == 1.0)
    def _():
        place(own)

    @pl.when(is_own != 1.0)
    def _():
        place(other)


def assemble(rows, own, other):
    vector = pl.BlockSpec(memory_space=pltpu.VMEM)
    main = pl.BlockSpec(memory_space=pltpu.MemorySpace.HBM)
    size, width = own[0].shape
    return pl.pallas_call(
        functools.partial(assemble_kernel, len(own)),
        out_shape=jax.ShapeDtypeStruct((size * len(own), width), own[0].dtype),
        in_specs=[vector] + [main] * (2 * len(own)),
        out_specs=vector,
        scratch_shapes=[pltpu.SemaphoreType.DMA((len(own),))],
        compiler_params=pltpu.CompilerParams(vmem_limit_bytes=8 * 2**20),
        name="assemble_shards",
    )(rows, *own, *other)


def collapsed(section_inputs, w_in, in_bias, w_out, out_bias, norm_gain, norm_bias, patches, plan):
    places = Plan(lax.axis_size("section"), lax.axis_size("tensor"))
    tensors, half = places.tensors, places.half
    place = lax.axis_index("section") * tensors + lax.axis_index("tensor")
    marks = lax.dynamic_slice_in_dim(jnp.array(places.marks(), jnp.float32), place, 1, 0)
    marks = jnp.broadcast_to(marks[0][:, None], (marks.shape[1], norm_gain.shape[1]))
    is_own = marks[0, 0] == 1.0

    slots = range(half)
    chunk = section_inputs.shape[1]
    everyone = range(places.sections)
    partner = places.partner_pairs()

    def spread(value):
        return [send(value, places.weight_pairs(slot)) for slot in slots]

    def shared(held, received):
        given = send(held, places.own_pairs(False))
        returned = send(received[0], places.own_pairs(True))
        own, other = [held, returned], [given, received[0]]
        for slot in range(1, half):
            swapped = send(received[slot], partner)
            own += [received[slot], swapped]
            other += [swapped, received[slot]]
        return assemble(rows, own, other)

    def tokens(value, sections):
        return [send(value, places.token_pairs(slot, sections)) for slot in slots]

    received_in = spread(w_in[0])
    received_out = spread(w_out[0])
    currents = tokens(section_inputs[0], everyone)
    selected = jnp.concatenate(
        [
            lax.dynamic_index_in_dim(patches, plan[tick_index], 0, keepdims=False)
            for tick_index in range(TICKS - 1)
        ],
        axis=0,
    )
    waiting = tokens(selected, [0])

    biases = [in_bias]
    for step in range(1, tensors):
        pairs = [((to + step) % tensors, to) for to in range(tensors)]
        biases.append(lax.ppermute(in_bias, "tensor", pairs))
    bias = jnp.concatenate(biases, axis=1).astype(jnp.float32)
    rows = jnp.concatenate([norm_gain, norm_bias, out_bias], axis=0)
    bias = jnp.where(is_own, bias, send(bias, partner))
    rows = jnp.where(is_own, rows, send(rows, partner))
    rows = jnp.concatenate([rows, marks], axis=0)
    full_in = shared(w_in[0], received_in)
    hiddens = [enter(currents[slot], rows, bias, full_in) for slot in slots]
    full_out = shared(w_out[0], received_out)
    operands = (rows, bias, full_in, full_out)

    def home(values, shift, near):
        return [send(values[slot], places.home_pairs(slot, shift, near)) for slot in slots]

    def hop(values):
        return [send(values[slot], places.hop_pairs()) for slot in slots]

    def blocks(tick_index, *kept):
        first_row = (tick_index - 1) * chunk
        made = []
        for slot in slots:
            chunks = [array[slot] for array in kept]
            made.append(run_block(first_row, currents[slot], waiting[slot], operands, chunks))
        return list(zip(*made))

    products = [leave(currents[slot], hiddens[slot], rows, full_out) for slot in slots]
    currents = hop(products)
    early = home(products, 1, False)
    arrivals = currents
    (products,) = blocks(1)
    currents = hop(products)
    made, boxed_products, boxed_arrivals = blocks(2, products, arrivals)
    currents = hop(made)
    late = home(boxed_products, 1, False)
    near = home(boxed_arrivals, 0, True)
    near_late = home(currents, 0, True)
    (products,) = blocks(3)
    final = home(products, 1, None)
    return collect(rows, early, late, near, near_late, final)[None]


def gathered(section_inputs, w_in, in_bias, w_out, out_bias, norm_gain, norm_bias, patches, plan):
    sections = lax.axis_size("section")
    section_index = lax.axis_index("section")
    gather = lambda value: lax.all_gather(value, "tensor", axis=0, tiled=True)
    full_in, full_bias, full_out = gather(w_in[0]), gather(in_bias[0]), gather(w_out[0])
    weights = [(full_in, full_bias.astype(jnp.float32), full_out)]
    current = section_inputs[0]
    records = []
    for tick_index in range(TICKS):
        produced = apply_block(current, weights, norm_gain[0], norm_bias[0], out_bias[0])
        pairs = [(source, (source + 1) % sections) for source in range(sections)]
        arrived = lax.ppermute(produced, "section", pairs)
        records.append(arrived)
        if tick_index + 1 < TICKS:
            selected = lax.dynamic_index_in_dim(patches, plan[tick_index], 0, keepdims=False)
            current = jnp.where(section_index == 0, selected, arrived)
    return jnp.stack(records, axis=0)[None]


def solution(mesh):
    sections, tensors = mesh.shape["section"], mesh.shape["tensor"]
    fits = sections % 2 == 0 and tensors % 2 == 0 and tensors <= sections // 2
    placed = (
        P("section", "tensor", None),
        P("section", "tensor", None),
        P("section", "tensor"),
        P("section", "tensor", None),
        P("section", None),
        P("section", None),
        P("section", None),
        P(None, "tensor", None),
        P(),
    )

    def body(*args):
        return (collapsed if fits else gathered)(*args)

    return jax.shard_map(
        body,
        mesh=mesh,
        in_specs=placed,
        out_specs=P("section", None, "tensor", None),
        check_vma=False,
    )
```

```python
import functools

import jax
import jax.numpy as jnp
from jax import lax
from jax.experimental import pallas as pl
from jax.experimental.pallas import tpu as pltpu
from jax.sharding import PartitionSpec as P


TICKS = 4


norm_floor = 0.1
gelu_slope = 1.702


class Plan:
    def __init__(self, sections, tensors):
        self.sections = sections
        self.tensors = tensors
        self.half = tensors // 2

    def side(self, section):
        return (section // 2 + section) % 2

    def stage(self, section):
        return self.half - 1 + self.side(section)

    def device(self, section, tensor):
        return section * self.tensors + tensor

    def worker(self, section, core):
        return self.device(section // 2 * 2 + core, self.stage(section))

    def weight_pairs(self, slot):
        return [
            (
                self.device(section, (self.stage(section) + step) % self.tensors),
                self.worker(section, (section + step) % 2),
            )
            for section in range(self.sections)
            for step in (2 * slot, 2 * slot + 1)
            if step > 0
        ]

    def own_pairs(self, back):
        pairs = [
            (self.worker(section, section % 2), self.worker(section, 1 - section % 2))
            for section in range(self.sections)
        ]
        return [(target, source) for source, target in pairs] if back else pairs

    def quarter(self, core, slot):
        return self.tensors - 1 - slot if core else slot

    def token_pairs(self, slot, sections):
        return [
            (self.device(section, self.quarter(core, slot)), self.worker(section, core))
            for section in sections
            for core in range(2)
        ]

    def partner_pairs(self):
        return [
            (self.worker(section, core), self.worker(section, 1 - core))
            for section in range(self.sections)
            for core in range(2)
        ]

    def hop_pairs(self):
        return [
            (self.worker(section, core), self.worker(section + 1, core))
            for section in range(self.sections - 1)
            for core in range(2)
        ]

    def kept_near(self, section, tensor):
        return section % 2 == 1 and (tensor >= self.half) == self.side(section)

    def home_pairs(self, slot, shift, near=None):
        pairs = []
        for section in range(self.sections):
            for core in range(2):
                tensor = self.quarter(core, slot)
                if near is None or self.kept_near(section, tensor) == near:
                    source = self.worker((section - shift) % self.sections, core)
                    pairs.append((source, self.device(section, tensor)))
        return pairs


    def marks(self):
        table = []
        for section in range(self.sections):
            for tensor in range(self.tensors):
                side = int(tensor >= self.half)
                own = (section // 2 + side) % 2
                slot = self.tensors - 1 - tensor if side else tensor
                first = section < 2 and own == 0
                near = self.kept_near(section, tensor)
                table.append([float(mark) for mark in (section % 2 == own, first, near, slot)])
        return table


def send(value, pairs):
    return lax.ppermute(value, ("section", "tensor"), pairs)


def normalize(current, gain_row, shift_row):
    widened = current.astype(jnp.float32)
    average = jnp.mean(widened, axis=-1, keepdims=True)
    centered = widened - average
    variance = jnp.mean(centered * centered, axis=-1, keepdims=True)
    normed = (centered * lax.rsqrt(variance + norm_floor) * gain_row + shift_row).astype(
        jnp.bfloat16
    )
    return (normed, widened)


def activate(preact):
    return preact * jax.nn.sigmoid(gelu_slope * preact)


def apply_block(current, weights, gain_row, shift_row, bias_row):
    normed, widened = normalize(current, gain_row, shift_row)
    total = None
    for rows_in, rows_bias, rows_out in weights:
        preact = lax.dot_general(
            normed, rows_in, (((1,), (1,)), ((), ())), preferred_element_type=jnp.float32
        )
        hidden = activate(preact + rows_bias).astype(jnp.bfloat16)
        part = jnp.dot(hidden, rows_out, preferred_element_type=jnp.float32)
        total = part if total is None else total + part
    return (widened + total + bias_row).astype(jnp.bfloat16)


GAIN, SHIFT, BIAS, OWN, FIRST, NEAR, SLOT = range(7)


def row(rows, index):
    return rows[index : index + 1, :]


def mark(rows, index):
    return jnp.max(row(rows, index))


def enter_kernel(arrived, rows, bias, rows_in, hidden):
    normed, _ = normalize(arrived[...], row(rows, GAIN), row(rows, SHIFT))
    preact = lax.dot_general(
        normed, rows_in[...], (((1,), (1,)), ((), ())), preferred_element_type=jnp.float32
    )
    hidden[...] = activate(preact + bias[...]).astype(jnp.bfloat16)


def leave_kernel(arrived, hidden, rows, rows_out, produced):
    total = jnp.dot(hidden[...], rows_out[...], preferred_element_type=jnp.float32)
    widened = arrived[...].astype(jnp.float32)
    produced[...] = (widened + total + row(rows, BIAS)).astype(jnp.bfloat16)


def enter(arrived, rows, bias, full_in):
    vector = pl.BlockSpec(memory_space=pltpu.VMEM)
    return pl.pallas_call(
        enter_kernel,
        out_shape=jax.ShapeDtypeStruct((arrived.shape[0], full_in.shape[0]), jnp.bfloat16),
        in_specs=[vector] * 4,
        out_specs=vector,
        compiler_params=pltpu.CompilerParams(vmem_limit_bytes=8 * 2**20),
        name="enter_block",
    )(arrived, rows, bias, full_in)


def leave(arrived, hidden, rows, full_out):
    vector = pl.BlockSpec(memory_space=pltpu.VMEM)
    return pl.pallas_call(
        leave_kernel,
        out_shape=jax.ShapeDtypeStruct(arrived.shape, arrived.dtype),
        in_specs=[vector] * 4,
        out_specs=vector,
        compiler_params=pltpu.CompilerParams(vmem_limit_bytes=8 * 2**20),
        name="leave_block",
    )(arrived, hidden, rows, full_out)


def block_kernel(first_row, box_products, arrived, fresh, rows, bias, rows_in, rows_out, *refs):
    size = arrived.shape[0]
    new = fresh[first_row : first_row + size, :].astype(jnp.float32)
    current = jnp.where(row(rows, FIRST) == 1.0, new, arrived[...].astype(jnp.float32))
    normed, widened = normalize(current, row(rows, GAIN), row(rows, SHIFT))
    preact = lax.dot_general(
        normed, rows_in[...], (((1,), (1,)), ((), ())), preferred_element_type=jnp.float32
    )
    hidden = activate(preact + bias[...]).astype(jnp.bfloat16)
    total = jnp.dot(hidden, rows_out[...], preferred_element_type=jnp.float32)
    result = (widened + total + row(rows, BIAS)).astype(jnp.bfloat16)
    if len(refs) == 1:
        refs[0][...] = result
        return
    kept, produced, box = refs
    produced[...] = result
    box[:size, :] = kept[...]
    box[size:, :] = result if box_products else arrived[...]


def run_block(first_row, arrived, fresh, operands, kept=(), box_products=False):
    vector = pl.BlockSpec(memory_space=pltpu.VMEM)
    size, width = arrived.shape
    chunks = [1, 2] if kept else [1]
    shapes = [jax.ShapeDtypeStruct((count * size, width), arrived.dtype) for count in chunks]
    return pl.pallas_call(
        functools.partial(block_kernel, first_row, box_products),
        out_shape=shapes,
        in_specs=[vector] * (6 + len(kept)),
        out_specs=[vector] * len(shapes),
        compiler_params=pltpu.CompilerParams(vmem_limit_bytes=8 * 2**20),
        name="section_block",
    )(arrived, fresh, *operands, *kept)


def collect_kernel(slots, rows, *refs):
    records = refs[-1]
    parts = [refs[index * slots : (index + 1) * slots] for index in range(5)]
    early, late, near, near_late, final = parts
    size = records.shape[1]
    ticks = records.shape[0]
    choice, is_near = mark(rows, SLOT), mark(rows, NEAR)

    def mine(part, start):
        value = part[0][start : start + size, :]
        for slot in range(1, slots):
            value = jnp.where(choice == slot, part[slot][start : start + size, :], value)
        return value

    def either(tick, far, far_start, close, close_start):
        records[tick] = jnp.where(is_near == 1.0, mine(close, close_start), mine(far, far_start))

    either(0, early, 0, near, 0)
    either(1, late, 0, near_late, 0)
    either(2, late, size, near_late, size)
    records[ticks - 1] = mine(final, 0)


def collect(rows, early, late, near, near_late, final):
    vector = pl.BlockSpec(memory_space=pltpu.VMEM)
    pieces = early + late + near + near_late + final
    return pl.pallas_call(
        functools.partial(collect_kernel, len(final)),
        out_shape=jax.ShapeDtypeStruct((TICKS,) + final[0].shape, final[0].dtype),
        in_specs=[vector] * (1 + len(pieces)),
        out_specs=vector,
        compiler_params=pltpu.CompilerParams(vmem_limit_bytes=8 * 2**20),
        name="collect_quarters",
    )(rows, *pieces)


def assemble_kernel(count, rows, *refs):
    own, other, full, done = refs[:count], refs[count : 2 * count], refs[-2], refs[-1]
    size = own[0].shape[0]

    def place(parts):
        copies = [
            pltpu.make_async_copy(part, full.at[pl.ds(step * size, size)], done.at[step])
            for step, part in enumerate(parts)
        ]
        for copy in copies:
            copy.start()
        for copy in copies:
            copy.wait()

    is_own = mark(rows, OWN)

    @pl.when(is_own == 1.0)
    def _():
        place(own)

    @pl.when(is_own != 1.0)
    def _():
        place(other)


def assemble(rows, own, other):
    vector = pl.BlockSpec(memory_space=pltpu.VMEM)
    main = pl.BlockSpec(memory_space=pltpu.MemorySpace.HBM)
    size, width = own[0].shape
    return pl.pallas_call(
        functools.partial(assemble_kernel, len(own)),
        out_shape=jax.ShapeDtypeStruct((size * len(own), width), own[0].dtype),
        in_specs=[vector] + [main] * (2 * len(own)),
        out_specs=vector,
        scratch_shapes=[pltpu.SemaphoreType.DMA((len(own),))],
        compiler_params=pltpu.CompilerParams(vmem_limit_bytes=8 * 2**20),
        name="assemble_shards",
    )(rows, *own, *other)


def collapsed(section_inputs, w_in, in_bias, w_out, out_bias, norm_gain, norm_bias, patches, plan):
    places = Plan(lax.axis_size("section"), lax.axis_size("tensor"))
    tensors, half = places.tensors, places.half
    place = lax.axis_index("section") * tensors + lax.axis_index("tensor")
    marks = lax.dynamic_slice_in_dim(jnp.array(places.marks(), jnp.float32), place, 1, 0)
    marks = jnp.broadcast_to(marks[0][:, None], (marks.shape[1], norm_gain.shape[1]))
    is_own = marks[0, 0] == 1.0

    slots = range(half)
    chunk = section_inputs.shape[1]
    everyone = range(places.sections)
    partner = places.partner_pairs()

    def spread(value):
        return [send(value, places.weight_pairs(slot)) for slot in slots]

    def shared(held, received):
        given = send(held, places.own_pairs(False))
        returned = send(received[0], places.own_pairs(True))
        own, other = [held, returned], [given, received[0]]
        for slot in range(1, half):
            swapped = send(received[slot], partner)
            own += [received[slot], swapped]
            other += [swapped, received[slot]]
        return assemble(rows, own, other)

    def tokens(value, sections):
        return [send(value, places.token_pairs(slot, sections)) for slot in slots]

    received_in = spread(w_in[0])
    received_out = spread(w_out[0])
    currents = tokens(section_inputs[0], everyone)
    selected = jnp.concatenate(
        [
            lax.dynamic_index_in_dim(patches, plan[tick_index], 0, keepdims=False)
            for tick_index in range(TICKS - 1)
        ],
        axis=0,
    )
    waiting = tokens(selected, [0])

    biases = [in_bias]
    for step in range(1, tensors):
        pairs = [((to + step) % tensors, to) for to in range(tensors)]
        biases.append(lax.ppermute(in_bias, "tensor", pairs))
    bias = jnp.concatenate(biases, axis=1).astype(jnp.float32)
    rows = jnp.concatenate([norm_gain, norm_bias, out_bias], axis=0)
    bias = jnp.where(is_own, bias, send(bias, partner))
    rows = jnp.where(is_own, rows, send(rows, partner))
    rows = jnp.concatenate([rows, marks], axis=0)
    full_in = shared(w_in[0], received_in)
    hiddens = [enter(currents[slot], rows, bias, full_in) for slot in slots]
    full_out = shared(w_out[0], received_out)
    operands = (rows, bias, full_in, full_out)

    def home(values, shift, near):
        return [send(values[slot], places.home_pairs(slot, shift, near)) for slot in slots]

    def hop(values):
        return [send(values[slot], places.hop_pairs()) for slot in slots]

    def blocks(tick_index, kept=(), box_products=False):
        first_row = (tick_index - 1) * chunk
        made = []
        for slot in slots:
            chunks = [kept[slot]] if kept else []
            made.append(
                run_block(first_row, currents[slot], waiting[slot], operands, chunks, box_products)
            )
        return [list(values) for values in zip(*made)]

    products = [leave(currents[slot], hiddens[slot], rows, full_out) for slot in slots]
    currents = hop(products)
    early = home(products, 1, False)
    near = home(currents, 0, True)
    (products,) = blocks(1)
    currents = hop(products)
    arrivals = currents
    products, boxed = blocks(2, products, True)
    currents = hop(products)
    late = home(boxed, 1, False)
    products, boxed = blocks(3, arrivals, False)
    final = home(products, 1, None)
    near_late = home(boxed, 0, True)
    return collect(rows, early, late, near, near_late, final)[None]


def gathered(section_inputs, w_in, in_bias, w_out, out_bias, norm_gain, norm_bias, patches, plan):
    sections = lax.axis_size("section")
    section_index = lax.axis_index("section")
    gather = lambda value: lax.all_gather(value, "tensor", axis=0, tiled=True)
    full_in, full_bias, full_out = gather(w_in[0]), gather(in_bias[0]), gather(w_out[0])
    weights = [(full_in, full_bias.astype(jnp.float32), full_out)]
    current = section_inputs[0]
    records = []
    for tick_index in range(TICKS):
        produced = apply_block(current, weights, norm_gain[0], norm_bias[0], out_bias[0])
        pairs = [(source, (source + 1) % sections) for source in range(sections)]
        arrived = lax.ppermute(produced, "section", pairs)
        records.append(arrived)
        if tick_index + 1 < TICKS:
            selected = lax.dynamic_index_in_dim(patches, plan[tick_index], 0, keepdims=False)
            current = jnp.where(section_index == 0, selected, arrived)
    return jnp.stack(records, axis=0)[None]


def solution(mesh):
    sections, tensors = mesh.shape["section"], mesh.shape["tensor"]
    fits = sections % 2 == 0 and tensors % 2 == 0 and tensors <= sections // 2
    placed = (
        P("section", "tensor", None),
        P("section", "tensor", None),
        P("section", "tensor"),
        P("section", "tensor", None),
        P("section", None),
        P("section", None),
        P("section", None),
        P(None, "tensor", None),
        P(),
    )

    def body(*args):
        return (collapsed if fits else gathered)(*args)

    return jax.shard_map(
        body,
        mesh=mesh,
        in_specs=placed,
        out_specs=P("section", None, "tensor", None),
        check_vma=False,
    )
```
